32 devices in a mesh: rep: 1, r: 8 (over y, z), s: 4 (over x, core).
Axes of the slice: x: 2, y: 2, z: 4, core: 2. Of those that a mesh axis runs over, the one named last changes fastest.
Arguments:
- x: bfloat16 [32, 4096, 512], P(('rep', 'r', 's'))
- dy: bfloat16 [32, 4096, 512], P(('rep', 'r', 's'))
- w_gate: bfloat16 [2, 512, 4096], P(None, 's')
- w_up: bfloat16 [2, 512, 4096], P(None, 's')
- w_down: bfloat16 [2, 4096, 512], P(None, 's')
- m_w_gate: float32 [2, 512, 4096], P(None, 's')
- m_w_up: float32 [2, 512, 4096], P(None, 's')
- m_w_down: float32 [2, 4096, 512], P(None, 's')
- v_w_gate: float32 [2, 512, 4096], P(None, 's')
- v_w_up: float32 [2, 512, 4096], P(None, 's')
- v_w_down: float32 [2, 4096, 512], P(None, 's')
Outputs:
- output 1: bfloat16 [2, 512, 4096], P('rep', 's')
- output 2: bfloat16 [2, 512, 4096], P('rep', 's')
- output 3: bfloat16 [2, 4096, 512], P('rep', 's')
- output 4: float32 [2, 512, 4096], P('rep', 's')
- output 5: float32 [2, 512, 4096], P('rep', 's')
- output 6: float32 [2, 4096, 512], P('rep', 's')
- output 7: float32 [2, 512, 4096], P('rep', 's')
- output 8: float32 [2, 512, 4096], P('rep', 's')
- output 9: float32 [2, 4096, 512], P('rep', 's')
All inputs are finite; a program needn't handle non-finite values.
Results may differ from the reference program's by a relative error of at most 0.022.
Values are sent between devices in bfloat16 or wider.
A program may use at most 2 GiB of HBM per device.

```python
import jax
import jax.numpy as jnp
from jax import lax

SEQUENCES = 32
TOKENS = 4096
D = 512
FF = 4096
LAYERS = 2
NAMES = ("w_gate", "w_up", "w_down")
SHAPES = {"w_gate": (LAYERS, D, FF), "w_up": (LAYERS, D, FF), "w_down": (LAYERS, FF, D)}


def bump(key, n, height):
    away = (jnp.arange(n, dtype=jnp.int32) - jax.random.randint(key, (), 0, n, jnp.int32)) % n
    return jnp.where(away < n // 8, height, 1.0)


def together(key, own, strength):
    shared = jax.random.normal(key, own.shape[1:], jnp.float32)
    return (own + strength * shared) * lax.rsqrt(1 + strength * strength)


def setup_inputs(seed: int = 0, part: int = 0) -> dict:
    kx, kdy, ka, kb, kz, kf, kh, kl, *keys = jax.random.split(jax.random.key(seed), 8 + 3 * len(NAMES))
    kx, kdy, ka, kb = (jax.random.fold_in(k, part) for k in (kx, kdy, ka, kb))
    kw, km, kv = (keys[i::3] for i in range(3))
    shape = (SEQUENCES, TOKENS, D)
    much_x, much_dy = jax.random.uniform(kz, (2,), jnp.float32, 0.0, 1.0)
    loud = 2.0 ** jax.random.uniform(jax.random.fold_in(kz, 1), (), jnp.float32, -1.0, 2.0)
    layers = 2.0 ** jax.random.uniform(kl, (LAYERS, 1, 1), jnp.float32, -1.0, 1.0)
    x = together(ka, jax.random.normal(kx, shape, jnp.float32), much_x) * bump(kf, D, 4.0)
    dy = together(kb, jax.random.normal(kdy, shape, jnp.float32), much_dy)
    drawn = {"x": x.astype(jnp.bfloat16), "dy": (loud * dy * (SEQUENCES * TOKENS) ** -0.5).astype(jnp.bfloat16)}
    for key, name in zip(kw, NAMES, strict=True):
        w = jax.random.normal(key, SHAPES[name], jnp.float32) * SHAPES[name][1] ** -0.5
        drawn[name] = (w * {"w_gate": 1.0, "w_up": bump(kh, FF, 4.0), "w_down": layers}[name]).astype(jnp.bfloat16)
    for key, name in zip(km, NAMES, strict=True):
        drawn[f"m_{name}"] = 0.1 * jax.random.normal(key, SHAPES[name], jnp.float32)
    for key, name in zip(kv, NAMES, strict=True):
        drawn[f"v_{name}"] = jax.random.uniform(key, SHAPES[name], jnp.float32, 0.005, 0.015)
    return drawn


def matmul(a, w):
    return jnp.dot(a, w, preferred_element_type=jnp.float32).astype(jnp.bfloat16)


def normed(h):
    wide = h.astype(jnp.float32)
    scale = lax.rsqrt(jnp.mean(wide**2, -1, keepdims=True) + 1e-6)
    return (wide * scale).astype(jnp.bfloat16)


def layer(h, w):
    a = normed(h)
    gate = jnp.dot(a, w["w_gate"], preferred_element_type=jnp.float32)
    up = jnp.dot(a, w["w_up"], preferred_element_type=jnp.float32)
    return h + matmul((jax.nn.silu(gate) * up).astype(jnp.bfloat16), w["w_down"])


def adamw(w, m, v, g):
    m = 0.9 * m + 0.1 * g
    v = 0.95 * v + 0.05 * g * g
    step = m * lax.rsqrt(v + 1e-8) + 0.1 * w
    return (w - 0.02 * step).astype(jnp.bfloat16), m, v


def clipped(gradients, sum_of_squares, count):
    factor = jnp.minimum(1.0, 0.5 * lax.rsqrt(sum_of_squares / count + 1e-30))
    return [g * factor for g in gradients]


def stack(weights, h):
    return lax.scan(lambda h, w: (layer(h, w), None), h, weights)[0]


def reference(x, dy, w_gate, w_up, w_down, m_w_gate, m_w_up, m_w_down, v_w_gate, v_w_up, v_w_down):
    weights = dict(zip(NAMES, (w_gate, w_up, w_down), strict=True))

    def take(so_far, sequence):
        h, by_y = sequence
        _, back = jax.vjp(lambda w: stack(w, h), weights)
        return jax.tree.map(lambda total, term: total + term.astype(jnp.float32), so_far, back(by_y)[0]), None

    none_yet = {name: jnp.zeros(w.shape, jnp.float32) for name, w in weights.items()}
    by_weights, _ = lax.scan(take, none_yet, (x, dy))
    gradients = [by_weights[name].astype(jnp.bfloat16).astype(jnp.float32) for name in NAMES]
    gradients = clipped(gradients, sum(jnp.sum(g * g) for g in gradients), sum(g.size for g in gradients))
    new = [
        adamw(w.astype(jnp.float32), m, v, g)
        for w, m, v, g in zip((w_gate, w_up, w_down), (m_w_gate, m_w_up, m_w_down), (v_w_gate, v_w_up, v_w_down), gradients, strict=True)
    ]
    return tuple(one[which] for which in range(3) for one in new)
```

```python
import functools

import jax
import jax.numpy as jnp
from jax import lax
from jax.experimental import pallas as pl
from jax.experimental.pallas import tpu as pltpu
from jax.sharding import PartitionSpec as P

MESH = pl.DeviceIdType.MESH
CHUNKS, CORES, XS, YS, ZS, OWNERS = 8, 2, 2, 2, 4, 4
f32, bf16 = jnp.float32, jnp.bfloat16


def dotn(a, b):
    return jnp.dot(a, b, preferred_element_type=f32)


def dott(a, b):
    return lax.dot_general(a, b, (((1,), (1,)), ((), ())), preferred_element_type=f32)


def dot0(a, b):
    return lax.dot_general(a, b, (((0,), (0,)), ((), ())), preferred_element_type=f32)


def kernel(
    sizes,
    x_hbm, dy_hbm, wg_hbm, wu_hbm, wd_hbm,
    gg_out, gu_out, gd_out, wbuf, a0_hbm,
    A, DH, H, total, W, act_s, du_s, dg_s, accs,
    sb0, rb0, own0, sb1, rb1, own1, sb2, rb2, own2, sb3, rb3, own3, gfin,
    in_sem, w_sem, out_sem,
    ws_send, wf_send, w_recv,
    s0, r0, s1, r1, s2, r2, s3, r3, s4, r4,
):
    T, D, F, Tt, rb, cb = sizes
    R = D // OWNERS
    HALF, QUARTER = R // YS, R // (YS * ZS)
    nt = T // Tt
    per = nt // 2
    me_r, me_s = lax.axis_index("r"), lax.axis_index("s")
    core, mx = lax.rem(me_s, CORES), me_s // CORES
    my, mz = me_r // ZS, lax.rem(me_r, ZS)
    partner = mx * CORES + 1 - core
    across = (1 - mx) * CORES + core
    to_partner = {"r": me_r, "s": partner}
    to_across = {"r": me_r, "s": across}
    to_y = {"r": (1 - my) * ZS + mz, "s": me_s}

    def remote(src, dst, send, recv, where):
        return pltpu.make_async_remote_copy(src, dst, send, recv, device_id=where, device_id_type=MESH)

    def rows(owner):
        return pl.ds(pl.multiple_of(owner * R, R), R)

    def own_pieces(l, j, into):
        wide = F // OWNERS
        for m, w in ((0, wg_hbm), (1, wu_hbm)):
            for o in range(OWNERS):
                cols = pl.ds(pl.multiple_of(o * wide * CHUNKS + j * wide, wide), wide)
                yield w.at[l, :, cols], into.at[m, rows(me_s), o * wide : (o + 1) * wide]
        yield wd_hbm.at[l, rows(j), :], into.at[2, rows(me_s), :]

    def send_own(c):
        l, j = c // CHUNKS, lax.rem(c, CHUNKS)
        for src, dst in own_pieces(l, j, wbuf.at[l, j]):
            remote(src, dst, ws_send.at[0, c], w_recv.at[0, c], to_across).start()
        for src, dst in own_pieces(l, j, wbuf.at[l, j]):
            remote(src, dst, ws_send.at[1, c], w_recv.at[1, c], to_partner).start()

    def package(c, owner):
        return wbuf.at[c // CHUNKS, lax.rem(c, CHUNKS), :, rows(owner), :]

    def wait_package(kind, c, owner):
        remote(package(c, owner), package(c, owner), wf_send.at[c], w_recv.at[kind, c], to_partner).wait_recv()

    def forward(c):
        wait_package(0, c, across)
        remote(package(c, across), package(c, across), wf_send.at[c], w_recv.at[2, c], to_partner).start()

    def load(n):
        slot = lax.rem(n, 2)
        l, j = lax.rem(n // CHUNKS, 2), lax.rem(n, CHUNKS)

        @pl.when(n < 2 * CHUNKS)
        def _():
            wait_package(1, n, partner)
            wait_package(2, n, (1 - mx) * CORES + 1 - core)

        for src, dst in own_pieces(l, j, W.at[slot]):
            pltpu.make_async_copy(src, dst, w_sem.at[slot]).start()
        for k in range(1, OWNERS):
            o = lax.rem(me_s + k, OWNERS)
            pltpu.make_async_copy(wbuf.at[l, j, :, rows(o), :], W.at[slot, :, rows(o), :], w_sem.at[slot]).start()

    def wait_load(n):
        slot = lax.rem(n, 2)
        pltpu.make_async_copy(wbuf.at[0, 0], W.at[slot], w_sem.at[slot]).wait()

    def g0(q):
        for m in range(3):
            for xx in range(XS):
                sb0[m, xx] = accs[m, rows(xx * CORES + 1 - core), :].astype(bf16)
        for m in range(3):
            for xx in range(XS):
                own0[m, xx] = accs[m, rows(xx * CORES + core), :]
        c0(q).start()

    def c0(q):
        return remote(sb0, rb0.at[lax.rem(q, 2)], s0, r0.at[lax.rem(q, 2)], to_partner)

    def g1(q):
        c0(q).wait()
        slot = lax.rem(q, 2)
        for m in range(3):
            sb1[m] = (own0[m, 1 - mx] + rb0[slot, m, 1 - mx].astype(f32)).astype(bf16)
        for m in range(3):
            own1[m] = own0[m, mx] + rb0[slot, m, mx].astype(f32)
        c1(q).start()

    def c1(q):
        return remote(sb1, rb1.at[lax.rem(q, 2)], s1, r1.at[lax.rem(q, 2)], to_across)

    def half(h):
        return pl.ds(pl.multiple_of(h * HALF, HALF), HALF)

    def g2(q):
        c1(q).wait()
        slot = lax.rem(q, 2)
        for m in range(3):
            sb2[m] = (own1[m, half(1 - my), :] + rb1[slot, m, half(1 - my), :].astype(f32)).astype(bf16)
        for m in range(3):
            own2[m] = own1[m, half(my), :] + rb1[slot, m, half(my), :].astype(f32)
        c2(q).start()

    def c2(q):
        return remote(sb2, rb2.at[lax.rem(q, 2)], s2, r2.at[lax.rem(q, 2)], to_y)

    def quarter(z):
        return pl.ds(pl.multiple_of(z * QUARTER, QUARTER), QUARTER)

    def c3(q, k):
        where = {"r": my * ZS + lax.rem(mz + 1 + k, ZS), "s": me_s}
        return remote(sb3.at[k], rb3.at[lax.rem(q, 2), k], s3.at[k], r3.at[lax.rem(q, 2), k], where)

    def g3(q):
        c2(q).wait()
        slot = lax.rem(q, 2)
        for k in range(ZS - 1):
            z = lax.rem(mz + 1 + k, ZS)
            for m in range(3):
                sb3[k, m] = (own2[m, quarter(z), :] + rb2[slot, m, quarter(z), :].astype(f32)).astype(bf16)
        for m in range(3):
            own3[m] = own2[m, quarter(mz), :] + rb2[slot, m, quarter(mz), :].astype(f32)
        for k in range(ZS - 1):
            c3(q, k).start()

    mine = pl.ds(pl.multiple_of(my * HALF + mz * QUARTER, QUARTER), QUARTER)

    def c4(q, k):
        part = gfin.at[q, :, mine, :]
        where = {"r": lax.rem(me_r + 1 + k, YS * ZS), "s": me_s}
        return remote(part, part, s4.at[q], r4.at[q], where)

    def all4(q):
        others = gfin.at[q, :, : R - QUARTER, :]
        return remote(others, others, s4.at[q], r4.at[q], to_y)

    def g4(q):
        slot = lax.rem(q, 2)
        for k in range(ZS - 1):
            c3(q, k).wait()
        for m in range(3):
            v = own3[m]
            for k in range(ZS - 1):
                v += rb3[slot, k, m].astype(f32)
            gfin[q, m, mine, :] = v.astype(bf16)
        for k in range(YS * ZS - 1):
            c4(q, k).start()

    def stores(q):
        l, j = 1 - q // CHUNKS, lax.rem(q, CHUNKS)
        wide = F // OWNERS
        for m, g in ((0, gg_out), (1, gu_out)):
            for o in range(OWNERS):
                cols = pl.ds(pl.multiple_of(o * wide * CHUNKS + j * wide, wide), wide)
                yield pltpu.make_async_copy(gfin.at[q, m, :, o * wide : (o + 1) * wide], g.at[l, :, cols], out_sem.at[q])
        yield pltpu.make_async_copy(gfin.at[q, 2], gd_out.at[l, rows(j), :], out_sem.at[q])

    def store(q):
        all4(q).wait()
        for copy in stores(q):
            copy.start()

    def when(test, what, q):
        pl.when(test)(lambda: what(q))

    last = 2 * CHUNKS

    def exchange(q, b):
        def at(stage, back, what):
            when((b == stage) & (q >= back) & (q < last + back), what, q - back)

        at(0, 4, store)
        at(0, 3, g4)
        at(0, 2, g2)
        at(0, 1, g0)
        at(1, 1, g1)
        at(2, 2, g3)

    def normed(wide):
        scale = lax.rsqrt(jnp.mean(wide * wide, -1, keepdims=True) + 1e-6)
        return (wide * scale).astype(bf16)

    def tile(t, n=Tt):
        return pl.ds(pl.multiple_of(t * n, n), n)

    def first(wslot, t, slot, backward, r, c):
        s = pl.ds(pl.multiple_of(t * Tt + r * rb, rb), rb)
        rs, cs = slice(r * rb, (r + 1) * rb), slice(c * cb, (c + 1) * cb)
        a = A[s, :]
        g = dotn(a, W[wslot, 0, :, cs])
        u = dotn(a, W[wslot, 1, :, cs])
        h = 0.5 * g
        th = jnp.tanh(h)
        silu = h * th + h
        if not backward:
            act_s[slot, rs, cs] = (silu * u).astype(bf16)
            return
        d = dott(DH[s, :], W[wslot, 2, cs, :]).astype(bf16).astype(f32)
        sig = 0.5 * th + 0.5
        act_s[slot, rs, cs] = (silu * u).astype(bf16)
        du_s[slot, rs, cs] = (d * silu).astype(bf16)
        dg_s[slot, rs, cs] = (d * u * (sig * (1.0 + g - silu))).astype(bf16)

    def second(wslot, t, slot, backward, input_too, begin, piece):
        s = tile(t)
        if not backward:
            total[s, :] += dotn(act_s[slot], W[wslot, 2])
            return
        if piece == 3:
            total[s, :] += dott(dg_s[slot], W[wslot, 0]) + dott(du_s[slot], W[wslot, 1])
            return
        if piece == 2:
            new = dot0(act_s[slot], DH[s, :])
        else:
            new = dot0(A[s, :], (dg_s, du_s)[piece][slot])
        if begin:
            accs[piece] = jnp.where(t == 0, 0.0, accs[piece]) + new
        else:
            accs[piece] += new

    blocks = [(r, c) for r in range(Tt // rb) for c in range(F // cb)]

    def together(w1, t1, slot1, w2, t2, slot2, backward, input_too, begin):
        pieces = list(range(4 if input_too else 3)) if backward else [0]
        done = 0
        for k, block in enumerate(blocks):
            first(w1, t1, slot1, backward, *block)
            while done < (k + 1) * len(pieces) // len(blocks):
                second(w2, t2, slot2, backward, input_too, begin, pieces[done])
                done += 1

    def phase(base, backward, input_too):
        for block in blocks:
            first(lax.rem(base, 2), 0, 0, backward, *block)

        def step(i, _):
            n, b = base + i // per, lax.rem(i, per)
            if backward:
                exchange(n - CHUNKS, b)
            if base < 2 * CHUNKS:
                when((b == 0) & (n + 4 < 2 * CHUNKS), send_own, n + 4)
                when((b == 0) & (n + 1 < 2 * CHUNKS), forward, n + 1)
            when((b == 1) & (n + 1 < 3 * CHUNKS), load, n + 1)
            when((b == per - 1) & (n + 1 < 3 * CHUNKS), wait_load, n + 1)
            w = lax.rem(n, 2)
            t = 2 * b
            together(w, t + 1, 1, w, t, 0, backward, input_too, True)
            over = b == per - 1
            together(jnp.where(over, 1 - w, w), jnp.where(over, 0, t + 2), 0, w, t + 1, 1, backward, input_too, False)
            return 0

        lax.fori_loop(0, per * CHUNKS, step, 0)

    barrier = pltpu.get_barrier_semaphore()
    peers = [to_partner, to_across] + [{"r": lax.rem(me_r + k, YS * ZS), "s": me_s} for k in range(1, YS * ZS)]
    for peer in peers:
        pl.semaphore_signal(barrier, inc=1, device_id=peer, device_id_type=MESH)
    load_x = pltpu.make_async_copy(x_hbm, H, in_sem.at[0])
    load_dy = pltpu.make_async_copy(dy_hbm, DH, in_sem.at[1])
    load_x.start()
    load_dy.start()
    pl.semaphore_wait(barrier, len(peers))
    lax.fori_loop(0, 4, lambda c, _: (send_own(c), 0)[1], 0)
    load_x.wait()

    def begin(t, _):
        s = tile(t, rb)
        A[s, :] = normed(H[s, :].astype(f32))
        total[s, :] = jnp.zeros((rb, D), f32)
        return 0

    lax.fori_loop(0, T // rb, begin, 0)
    save_a = pltpu.make_async_copy(A, a0_hbm, in_sem.at[0])
    save_a.start()
    forward(0)
    load(0)
    wait_load(0)
    phase(0, False, False)
    save_a.wait()
    load_dy.wait()

    def between(t, _):
        s = tile(t, rb)
        h = (H[s, :].astype(f32) + total[s, :].astype(bf16).astype(f32)).astype(bf16)
        H[s, :] = h
        A[s, :] = normed(h.astype(f32))
        total[s, :] = jnp.zeros((rb, D), f32)
        return 0

    lax.fori_loop(0, T // rb, between, 0)
    phase(CHUNKS, True, True)
    load_a = pltpu.make_async_copy(a0_hbm, A, in_sem.at[0])
    load_a.start()

    def back(t, _):
        s = tile(t, rb)
        wide = H[s, :].astype(f32)
        da = total[s, :].astype(bf16).astype(f32)
        scale = lax.rsqrt(jnp.mean(wide * wide, -1, keepdims=True) + 1e-6)
        along = jnp.sum(da * wide, -1, keepdims=True) * (scale * scale * scale * (1.0 / D))
        dn = (da * scale - wide * along).astype(bf16).astype(f32)
        DH[s, :] = (DH[s, :].astype(f32) + dn).astype(bf16)
        return 0

    lax.fori_loop(0, T // rb, back, 0)
    load_a.wait()
    phase(2 * CHUNKS, True, False)

    def drain(i, _):
        exchange(last + i // per, lax.rem(i, per))
        return 0

    lax.fori_loop(0, 4 * per, drain, 0)

    def finish(q, _):
        for copy in stores(q):
            copy.wait()
        l, j = q // CHUNKS, lax.rem(q, CHUNKS)
        two = wbuf.at[l, j, :, : R, :]
        for k in range(2):
            remote(two, two, ws_send.at[k, q], w_recv.at[0, q], to_partner).wait_send()
        remote(two, two, wf_send.at[q], w_recv.at[0, q], to_partner).wait_send()
        return 0

    lax.fori_loop(0, last, finish, 0)


def gradients_of(x, dy, w_gate, w_up, w_down, tiles=(512, 256, 256), vmem=63 * 2**20):
    T, D = x.shape
    F = w_gate.shape[2] // CHUNKS
    Tt, rb, cb = tiles
    R = D // OWNERS
    H, Q = R // YS, R // (YS * ZS)
    n = 2 * CHUNKS
    vm = pltpu.VMEM
    dma, any_ = pltpu.SemaphoreType.DMA, pl.BlockSpec(memory_space=pl.ANY)
    shape = jax.ShapeDtypeStruct
    outs = pl.pallas_call(
        functools.partial(kernel, (T, D, F, Tt, rb, cb)),
        in_specs=[any_] * 5,
        out_specs=[any_] * 5,
        out_shape=[shape(w.shape, bf16) for w in (w_gate, w_up, w_down)]
        + [shape((2, CHUNKS, 3, D, F), bf16), shape((T, D), bf16)],
        scratch_shapes=[
            vm((T, D), bf16), vm((T, D), bf16), vm((T, D), bf16), vm((T, D), f32),
            vm((2, 3, D, F), bf16), vm((2, Tt, F), bf16), vm((2, Tt, F), bf16), vm((2, Tt, F), bf16), vm((3, D, F), f32),
            vm((3, XS, R, F), bf16), vm((2, 3, XS, R, F), bf16), vm((3, XS, R, F), f32),
            vm((3, R, F), bf16), vm((2, 3, R, F), bf16), vm((3, R, F), f32),
            vm((3, H, F), bf16), vm((2, 3, H, F), bf16), vm((3, H, F), f32),
            vm((ZS - 1, 3, Q, F), bf16), vm((2, ZS - 1, 3, Q, F), bf16), vm((3, Q, F), f32),
            vm((n, 3, R, F), bf16),
            dma((2,)), dma((2,)), dma((n,)),
            dma((2, n)), dma((n,)), dma((3, n)),
            dma, dma((2,)), dma, dma((2,)), dma, dma((2,)), dma((ZS - 1,)), dma((2, ZS - 1)), dma((n,)), dma((n,)),
        ],
        compiler_params=pltpu.CompilerParams(collective_id=0, has_side_effects=True, vmem_limit_bytes=vmem),
    )(x, dy, w_gate, w_up, w_down)
    return outs[:3]


def adamw(w, m, v, g):
    m = 0.9 * m + 0.1 * g
    v = 0.95 * v + 0.05 * g * g
    step = m * lax.rsqrt(v + 1e-8) + 0.1 * w
    return (w - 0.02 * step).astype(bf16), m, v


def clipped(gradients, sum_of_squares, count):
    factor = jnp.minimum(1.0, 0.5 * lax.rsqrt(sum_of_squares / count + 1e-30))
    return [g * factor for g in gradients]


def solution(mesh, **options):
    def step(x, dy, *arrays):
        weights, m, v = (arrays[i : i + 3] for i in (0, 3, 6))
        gradients = [g.astype(f32) for g in gradients_of(x[0], dy[0], *weights, **options)]
        squares = lax.psum(sum(jnp.sum(g * g) for g in gradients), "s")
        gradients = clipped(gradients, squares, lax.psum(1, "s") * sum(g.size for g in gradients))
        new = [adamw(w.astype(f32), m, v, g) for w, m, v, g in zip(weights, m, v, gradients, strict=True)]
        return tuple(one[which] for which in range(3) for one in new)

    states, cut = P(("rep", "r", "s"), None, None), P(None, "s", None)
    return jax.shard_map(
        step,
        mesh=mesh,
        in_specs=(states, states) + (cut,) * 9,
        out_specs=(P("rep", "s", None),) * 9,
        check_vma=False,
    )
```

```python
import functools

import jax
import jax.numpy as jnp
from jax import lax
from jax.experimental import pallas as pl
from jax.experimental.pallas import tpu as pltpu
from jax.sharding import PartitionSpec as P

MESH = pl.DeviceIdType.MESH
CHUNKS, CORES, XS, YS, ZS, OWNERS = 8, 2, 2, 2, 4, 4
f32, bf16 = jnp.float32, jnp.bfloat16

EARLY = ((1, 0), (1, 1), (1, 2), (2, 0), (2, 1))


def dotn(a, b):
    return jnp.dot(a, b, preferred_element_type=f32)


def dott(a, b):
    return lax.dot_general(a, b, (((1,), (1,)), ((), ())), preferred_element_type=f32)


def dot0(a, b):
    return lax.dot_general(a, b, (((0,), (0,)), ((), ())), preferred_element_type=f32)


def kernel(
    sizes,
    x_hbm, dy_hbm, wg_hbm, wu_hbm, wd_hbm, *refs,
):
    early, refs = refs[: len(EARLY)], refs[len(EARLY) :]
    kernel_(sizes, x_hbm, dy_hbm, wg_hbm, wu_hbm, wd_hbm, early, refs[4 : 4 + len(EARLY)], *refs[:4], *refs[4 + len(EARLY) :])


def kernel_(
    sizes,
    x_hbm, dy_hbm, wg_hbm, wu_hbm, wd_hbm, early, early_out, gfin, factor, wbuf, a0_hbm,
    A, DH, H, total, W, act_s, du_s, dg_s, accs,
    sb0, rb0, own0, sb1, rb1, own1, sb2, rb2, own2, sb3, rb3, own3, piece, squares, over_r, over_s,
    in_sem, early_sem, w_sem, out_sem,
    ws_send, wf_send, w_recv,
    s0, r0, s1, r1, s2, r2, s3, r3, s4, r4, s5, r5, sn, rn, sm, rm,
):
    T, D, F, Tt, rb, cb, LANES = sizes
    COUNT = 2 * CHUNKS * 3 * D * F
    R = D // OWNERS
    HALF, QUARTER = R // YS, R // (YS * ZS)
    nt = T // Tt
    per = nt // 2
    me_r, me_s = lax.axis_index("r"), lax.axis_index("s")
    core, mx = lax.rem(me_s, CORES), me_s // CORES
    my, mz = me_r // ZS, lax.rem(me_r, ZS)
    partner = mx * CORES + 1 - core
    across = (1 - mx) * CORES + core
    to_partner = {"r": me_r, "s": partner}
    to_across = {"r": me_r, "s": across}
    to_y = {"r": (1 - my) * ZS + mz, "s": me_s}

    def remote(src, dst, send, recv, where):
        return pltpu.make_async_remote_copy(src, dst, send, recv, device_id=where, device_id_type=MESH)

    def rows(owner):
        return pl.ds(pl.multiple_of(owner * R, R), R)

    def own_pieces(l, j, into):
        wide = F // OWNERS
        for m, w in ((0, wg_hbm), (1, wu_hbm)):
            for o in range(OWNERS):
                cols = pl.ds(pl.multiple_of(o * wide * CHUNKS + j * wide, wide), wide)
                yield w.at[l, :, cols], into.at[m, rows(me_s), o * wide : (o + 1) * wide]
        yield wd_hbm.at[l, rows(j), :], into.at[2, rows(me_s), :]

    def send_own(c):
        l, j = c // CHUNKS, lax.rem(c, CHUNKS)
        for src, dst in own_pieces(l, j, wbuf.at[l, j]):
            remote(src, dst, ws_send.at[0, c], w_recv.at[0, c], to_across).start()
        for src, dst in own_pieces(l, j, wbuf.at[l, j]):
            remote(src, dst, ws_send.at[1, c], w_recv.at[1, c], to_partner).start()

    def package(c, owner):
        return wbuf.at[c // CHUNKS, lax.rem(c, CHUNKS), :, rows(owner), :]

    def wait_package(kind, c, owner):
        remote(package(c, owner), package(c, owner), wf_send.at[c], w_recv.at[kind, c], to_partner).wait_recv()

    def forward(c):
        wait_package(0, c, across)
        remote(package(c, across), package(c, across), wf_send.at[c], w_recv.at[2, c], to_partner).start()

    def load(n):
        slot = lax.rem(n, 2)
        l, j = lax.rem(n // CHUNKS, 2), lax.rem(n, CHUNKS)

        @pl.when(n < 2 * CHUNKS)
        def _():
            wait_package(1, n, partner)
            wait_package(2, n, (1 - mx) * CORES + 1 - core)

        for src, dst in own_pieces(l, j, W.at[slot]):
            pltpu.make_async_copy(src, dst, w_sem.at[slot]).start()
        for k in range(1, OWNERS):
            o = lax.rem(me_s + k, OWNERS)
            pltpu.make_async_copy(wbuf.at[l, j, :, rows(o), :], W.at[slot, :, rows(o), :], w_sem.at[slot]).start()

    def wait_load(n):
        slot = lax.rem(n, 2)
        pltpu.make_async_copy(wbuf.at[0, 0], W.at[slot], w_sem.at[slot]).wait()

    def c0(q, m):
        slot = lax.rem(q, 2)
        return remote(sb0.at[m], rb0.at[slot, m], s0.at[m], r0.at[slot, m], to_partner)

    def g0(q, m):
        for xx in range(XS):
            sb0[m, xx] = accs[m, rows(xx * CORES + 1 - core), :].astype(bf16)
        for xx in range(XS):
            own0[m, xx] = accs[m, rows(xx * CORES + core), :]
        c0(q, m).start()

    def c1(q, m):
        slot = lax.rem(q, 2)
        return remote(sb1.at[m], rb1.at[slot, m], s1.at[m], r1.at[slot, m], to_across)

    def g1(q, m):
        c0(q, m).wait()
        slot = lax.rem(q, 2)
        sb1[m] = (own0[m, 1 - mx] + rb0[slot, m, 1 - mx].astype(f32)).astype(bf16)
        own1[m] = own0[m, mx] + rb0[slot, m, mx].astype(f32)
        c1(q, m).start()

    def half(h):
        return pl.ds(pl.multiple_of(h * HALF, HALF), HALF)

    def c2(q, m):
        slot = lax.rem(q, 2)
        return remote(sb2.at[m], rb2.at[slot, m], s2.at[m], r2.at[slot, m], to_y)

    def g2(q, m):
        c1(q, m).wait()
        slot = lax.rem(q, 2)
        sb2[m] = (own1[m, half(1 - my), :] + rb1[slot, m, half(1 - my), :].astype(f32)).astype(bf16)
        own2[m] = own1[m, half(my), :] + rb1[slot, m, half(my), :].astype(f32)
        c2(q, m).start()

    def quarter(z):
        return pl.ds(pl.multiple_of(z * QUARTER, QUARTER), QUARTER)

    def c3(q, m, k):
        where = {"r": my * ZS + lax.rem(mz + 1 + k, ZS), "s": me_s}
        slot = lax.rem(q, 2)
        return remote(sb3.at[m, k], rb3.at[slot, m, k], s3.at[m, k], r3.at[slot, m, k], where)

    def g3(q, m):
        c2(q, m).wait()
        slot = lax.rem(q, 2)
        for k in range(ZS - 1):
            z = lax.rem(mz + 1 + k, ZS)
            sb3[m, k] = (own2[m, quarter(z), :] + rb2[slot, m, quarter(z), :].astype(f32)).astype(bf16)
        own3[m] = own2[m, quarter(mz), :] + rb2[slot, m, quarter(mz), :].astype(f32)
        for k in range(ZS - 1):
            c3(q, m, k).start()

    mine = pl.ds(pl.multiple_of(my * HALF + mz * QUARTER, QUARTER), QUARTER)

    def to_peer(k):
        return {"r": lax.rem(me_r + 1 + k, YS * ZS), "s": me_s}

    def c4(q, m, k):
        where = {"r": my * ZS + lax.rem(mz + 1 + k, ZS), "s": me_s}
        return remote(piece.at[q, m], gfin.at[q, m, mine, :], s4.at[q, m], r4.at[q, m], where)

    def c4_here(q, m):
        return pltpu.make_async_copy(piece.at[q, m], gfin.at[q, m, mine, :], out_sem.at[q, m])

    def g4(q, m):
        slot = lax.rem(q, 2)
        for k in range(ZS - 1):
            c3(q, m, k).wait()
        v = own3[m]
        for k in range(ZS - 1):
            v += rb3[slot, m, k].astype(f32)
        v = v.astype(bf16)
        piece[q, m] = v
        v = v.astype(f32)
        squares[...] += sum(v[:, i : i + LANES] * v[:, i : i + LANES] for i in range(0, F, LANES))
        for k in range(ZS - 1):
            c4(q, m, k).start()
        c4_here(q, m).start()

    def c5(q, m):
        part = gfin.at[q, m, half(my), :]
        return remote(part, part, s5.at[q, m], r5.at[q, m], to_y)

    def g5(q, m):
        others = gfin.at[q, m, : HALF - QUARTER, :]
        remote(others, others, s4.at[q, m], r4.at[q, m], to_y).wait()
        c4_here(q, m).wait()
        c5(q, m).start()

    def each(stage, which=(0, 1, 2)):
        def run(q):
            for m in which:
                stage(q, m)

        run.__name__ = stage.__name__
        return run

    def when(test, what, q):
        def run():
            with jax.named_scope(what.__name__):
                what(q)
        pl.when(test)(run)

    last = 2 * CHUNKS

    def exchange(q, b):
        def at(stage, back, what, which=(0, 1, 2)):
            when((b == stage) & (q >= back), each(what, which), q - back)

        at(0, 2, g2, (2,))
        at(0, 1, g0)
        at(0, 3, g4, (2,))
        at(1, 1, g1)
        at(1, 2, g3, (0, 1))
        at(1, 3, g5, (0, 1))
        at(2, 2, g3, (2,))
        at(2, 3, g5, (2,))
        at(3, 1, g2, (0, 1))
        at(3, 2, g4, (0, 1))

    def drain():
        a, b, c = last - 3, last - 2, last - 1
        each(g0)(c)
        g2(b, 2)
        g4(a, 2)
        each(g3, (0, 1))(b)
        each(g1)(c)
        each(g5, (0, 1))(a)
        g3(b, 2)
        each(g4, (0, 1))(b)
        g5(a, 2)
        g2(c, 0)
        g4(b, 2)
        g2(c, 1)
        g3(c, 0)
        each(g5, (0, 1))(b)
        g2(c, 2)
        g3(c, 1)
        g5(b, 2)
        g4(c, 0)
        g3(c, 2)
        g4(c, 1)
        g5(c, 0)
        g4(c, 2)
        over_r[me_r] = squares[...]
        peers_r = [to_peer(k) for k in range(YS * ZS - 1)]
        from_r = [lax.rem(me_r + YS * ZS - 1 - k, YS * ZS) for k in range(YS * ZS - 1)]
        peers_s = [{"r": me_r, "s": lax.rem(me_s + 1 + k, OWNERS)} for k in range(OWNERS - 1)]
        from_s = [lax.rem(me_s + OWNERS - 1 - k, OWNERS) for k in range(OWNERS - 1)]
        tell(me_r, over_r, sn, rn, peers_r)
        g5(c, 1)
        hear(me_r, over_r, sn, rn, peers_r, from_r)
        over_s[me_s] = jnp.sum(over_r[...], 0)
        tell(me_s, over_s, sm, rm, peers_s)
        g5(c, 2)
        hear(me_s, over_s, sm, rm, peers_s, from_s)

    def tell(me, scratch, send, recv, others):
        for k, where in enumerate(others):
            remote(scratch.at[me], scratch.at[me], send.at[k], recv.at[k], where).start()

    def hear(me, scratch, send, recv, others, places):
        for k, (where, place) in enumerate(zip(others, places)):
            remote(scratch.at[me], scratch.at[place], send.at[k], recv.at[k], where).wait()

    def normed(wide):
        scale = lax.rsqrt(jnp.mean(wide * wide, -1, keepdims=True) + 1e-6)
        return (wide * scale).astype(bf16)

    def tile(t, n=Tt):
        return pl.ds(pl.multiple_of(t * n, n), n)

    def first(wslot, t, slot, backward, r, c):
        s = pl.ds(pl.multiple_of(t * Tt + r * rb, rb), rb)
        rs, cs = slice(r * rb, (r + 1) * rb), slice(c * cb, (c + 1) * cb)
        a = A[s, :]
        g = dotn(a, W[wslot, 0, :, cs])
        u = dotn(a, W[wslot, 1, :, cs])
        h = 0.5 * g
        th = jnp.tanh(h)
        silu = h * th + h
        if not backward:
            act_s[slot, rs, cs] = (silu * u).astype(bf16)
            return
        d = dott(DH[s, :], W[wslot, 2, cs, :]).astype(bf16).astype(f32)
        sig = 0.5 * th + 0.5
        act_s[slot, rs, cs] = (silu * u).astype(bf16)
        du_s[slot, rs, cs] = (d * silu).astype(bf16)
        dg_s[slot, rs, cs] = (d * u * (sig * (1.0 + g - silu))).astype(bf16)

    def second(wslot, t, slot, backward, input_too, begin, which):
        s = tile(t)
        if not backward:
            total[s, :] += dotn(act_s[slot], W[wslot, 2])
            return
        if which == 3:
            total[s, :] += dott(dg_s[slot], W[wslot, 0]) + dott(du_s[slot], W[wslot, 1])
            return
        if which == 2:
            new = dot0(act_s[slot], DH[s, :])
        else:
            new = dot0(A[s, :], (dg_s, du_s)[which][slot])
        if begin:
            accs[which] = jnp.where(t == 0, 0.0, accs[which]) + new
        else:
            accs[which] += new

    blocks = [(r, c) for r in range(Tt // rb) for c in range(F // cb)]

    def together(w1, t1, slot1, w2, t2, slot2, backward, input_too, begin):
        for which in range(4 if input_too else 3) if backward else [0]:
            second(w2, t2, slot2, backward, input_too, begin, which)
        for block in blocks:
            first(w1, t1, slot1, backward, *block)

    def phase(base, backward, input_too):
        for block in blocks:
            first(lax.rem(base, 2), 0, 0, backward, *block)

        def step(i, _):
            n, b = base + i // per, lax.rem(i, per)
            if backward:
                exchange(n - CHUNKS, b)
            if base < 2 * CHUNKS:
                when((b == 0) & (n + 4 < 2 * CHUNKS), send_own, n + 4)
                when((b == 1) & (n + 1 < 2 * CHUNKS), forward, n + 1)
            when((b == 2) & (n + 1 < 3 * CHUNKS), load, n + 1)
            when((b == per - 1) & (n + 1 < 3 * CHUNKS), wait_load, n + 1)
            w = lax.rem(n, 2)
            t = 2 * b
            together(w, t + 1, 1, w, t, 0, backward, input_too, True)
            over = b == per - 1
            together(jnp.where(over, 1 - w, w), jnp.where(over, 0, t + 2), 0, w, t + 1, 1, backward, input_too, False)
            return 0

        lax.fori_loop(0, per * CHUNKS, step, 0)

    barrier = pltpu.get_barrier_semaphore()
    peers = [to_partner, to_across] + [{"r": lax.rem(me_r + k, YS * ZS), "s": me_s} for k in range(1, YS * ZS)]
    for peer in peers:
        pl.semaphore_signal(barrier, inc=1, device_id=peer, device_id_type=MESH)
    load_x = pltpu.make_async_copy(x_hbm, H, in_sem.at[0])
    load_dy = pltpu.make_async_copy(dy_hbm, DH, in_sem.at[1])
    load_x.start()
    load_dy.start()
    with jax.named_scope('barrier'):
        pl.semaphore_wait(barrier, len(peers))
    lax.fori_loop(0, 4, lambda c, _: (send_own(c), 0)[1], 0)
    load_x.wait()

    def begin(t, _):
        s = tile(t, rb)
        A[s, :] = normed(H[s, :].astype(f32))
        total[s, :] = jnp.zeros((rb, D), f32)
        return 0

    squares[...] = jnp.zeros(squares.shape, f32)
    with jax.named_scope('begin'):
        lax.fori_loop(0, T // rb, begin, 0)
    save_a = pltpu.make_async_copy(A, a0_hbm, in_sem.at[0])
    save_a.start()
    with jax.named_scope('first_load'):
        forward(0)
        load(0)
        wait_load(0)
    with jax.named_scope('p_fwd'):
        phase(0, False, False)
    save_a.wait()
    load_dy.wait()

    def between(t, _):
        s = tile(t, rb)
        h = (H[s, :].astype(f32) + total[s, :].astype(bf16).astype(f32)).astype(bf16)
        H[s, :] = h
        A[s, :] = normed(h.astype(f32))
        total[s, :] = jnp.zeros((rb, D), f32)
        return 0

    with jax.named_scope('between'):
        lax.fori_loop(0, T // rb, between, 0)
    with jax.named_scope('p_one'):
        phase(CHUNKS, True, True)
    load_a = pltpu.make_async_copy(a0_hbm, A, in_sem.at[0])
    load_a.start()

    def back(t, _):
        s = tile(t, rb)
        wide = H[s, :].astype(f32)
        da = total[s, :].astype(bf16).astype(f32)
        scale = lax.rsqrt(jnp.mean(wide * wide, -1, keepdims=True) + 1e-6)
        along = jnp.sum(da * wide, -1, keepdims=True) * (scale * scale * scale * (1.0 / D))
        dn = (da * scale - wide * along).astype(bf16).astype(f32)
        DH[s, :] = (DH[s, :].astype(f32) + dn).astype(bf16)
        return 0

    with jax.named_scope('back'):
        lax.fori_loop(0, T // rb, back, 0)
        load_a.wait()
    fetch = [pltpu.make_async_copy(src, dst, early_sem.at[i]) for i, (src, dst) in enumerate(zip(early, early_out))]
    for copy in fetch:
        copy.start()
    with jax.named_scope('p_zero'):
        phase(2 * CHUNKS, True, False)

    with jax.named_scope("drain"):
        drain()
    with jax.named_scope("norm"):
        mean = jnp.sum(over_s[...]) * (1.0 / COUNT)
        factor[...] = jnp.minimum(1.0, 0.5 * lax.rsqrt(jnp.full(factor.shape, mean + 1e-30, f32)))

    def finish(q, _):
        for m in range(3):
            c5(q, m).wait()
        l, j = q // CHUNKS, lax.rem(q, CHUNKS)
        two = wbuf.at[l, j, :, : R, :]
        for k in range(2):
            remote(two, two, ws_send.at[k, q], w_recv.at[0, q], to_partner).wait_send()
        remote(two, two, wf_send.at[q], w_recv.at[0, q], to_partner).wait_send()
        return 0

    for copy in fetch:
        copy.wait()
    with jax.named_scope('finish'):
        lax.fori_loop(0, last, finish, 0)


def gradients_of(x, dy, w_gate, w_up, w_down, early, tiles=(512, 256, 256), vmem=41 * 2**20):
    T, D = x.shape
    F = w_gate.shape[2] // CHUNKS
    Tt, rb, cb = tiles
    R = D // OWNERS
    H, Q = R // YS, R // (YS * ZS)
    n = 2 * CHUNKS
    lanes = min(F, 128)
    vm = pltpu.VMEM
    dma, hbm = pltpu.SemaphoreType.DMA, pl.BlockSpec(memory_space=pltpu.HBM)
    outs = pl.pallas_call(
        functools.partial(kernel, (T, D, F, Tt, rb, cb, lanes)),
        in_specs=[hbm] * (5 + len(early)),
        out_specs=[hbm, pl.BlockSpec(memory_space=pltpu.VMEM), hbm, hbm] + [pl.BlockSpec(memory_space=pltpu.VMEM)] * len(early),
        out_shape=[
            pltpu.HBM((n, 3, R, F), bf16), pltpu.VMEM((8, 128), f32),
            pltpu.HBM((2, CHUNKS, 3, D, F), bf16), pltpu.HBM((T, D), bf16),
            *(pltpu.VMEM(a.shape, a.dtype) for a in early),
        ],
        scratch_shapes=[
            vm((T, D), bf16), vm((T, D), bf16), vm((T, D), bf16), vm((T, D), f32),
            vm((2, 3, D, F), bf16), vm((2, Tt, F), bf16), vm((2, Tt, F), bf16), vm((2, Tt, F), bf16), vm((3, D, F), f32),
            vm((3, XS, R, F), bf16), vm((2, 3, XS, R, F), bf16), vm((3, XS, R, F), f32),
            vm((3, R, F), bf16), vm((2, 3, R, F), bf16), vm((3, R, F), f32),
            vm((3, H, F), bf16), vm((2, 3, H, F), bf16), vm((3, H, F), f32),
            vm((3, ZS - 1, Q, F), bf16), vm((2, 3, ZS - 1, Q, F), bf16), vm((3, Q, F), f32),
            vm((n, 3, Q, F), bf16), vm((Q, lanes), f32), vm((YS * ZS, Q, lanes), f32), vm((OWNERS, Q, lanes), f32),
            dma((2,)), dma((len(early),)), dma((2,)), dma((n, 3)),
            dma((2, n)), dma((n,)), dma((3, n)),
            dma((3,)), dma((2, 3)), dma((3,)), dma((2, 3)), dma((3,)), dma((2, 3)), dma((3, ZS - 1)), dma((2, 3, ZS - 1)), dma((n, 3)), dma((n, 3)), dma((n, 3)), dma((n, 3)),
            dma((YS * ZS - 1,)), dma((YS * ZS - 1,)), dma((OWNERS - 1,)), dma((OWNERS - 1,)),
        ],
        compiler_params=pltpu.CompilerParams(collective_id=0, has_side_effects=True, vmem_limit_bytes=vmem),
    )(*(pltpu.with_memory_space_constraint(a, pltpu.HBM) for a in (x, dy, w_gate, w_up, w_down, *early)))
    return outs[0], outs[1], outs[4:]


def update(factor, ga, gb, gc, *refs):
    l, o = pl.program_id(0), pl.program_id(1)
    scale = factor[0:1, 0:1]
    for i, g in enumerate((ga, gb, gc)):
        _, parts, _, R, wide = g.shape
        size = wide if i < 2 else R
        for j in range(parts):
            near = slice(j * size, (j + 1) * size)
            far = pl.ds(pl.multiple_of((o * parts + j) * size, size), size)

            def read(kind):
                ref, layer, cut = (refs[3 * kind + i], l, far) if (kind, i) in EARLY else (refs[3 * kind + i], 0, near)
                return ref[layer, :, cut] if i < 2 else ref[layer, cut, :]

            def write(kind, value):
                if i < 2:
                    refs[9 + 3 * kind + i][0, :, near] = value
                else:
                    refs[9 + 3 * kind + i][0, near, :] = value

            gradient = g[0, j, 0].astype(f32) * scale
            m = 0.9 * read(1) + 0.1 * gradient
            v = 0.95 * read(2) + 0.05 * gradient * gradient
            w = read(0).astype(f32)
            write(0, (w - 0.02 * (m * lax.rsqrt(v + 1e-8) + 0.1 * w)).astype(bf16))
            write(1, m)
            write(2, v)


def updated(g, factor, weights, m, v):
    _, _, _, R, F = g.shape
    wide = F // OWNERS
    at = pl.BlockSpec
    native = [at((1, R, CHUNKS * wide), lambda l, o: (l, 0, o))] * 2 + [at((1, CHUNKS * R // OWNERS, F), lambda l, o: (l, o, 0))]
    mine = [at((1, CHUNKS, 1, R, wide), lambda l, o, k=k: (1 - l, 0, k, 0, o)) for k in range(2)]
    mine.append(at((1, CHUNKS // OWNERS, 1, R, F), lambda l, o: (1 - l, o, 2, 0, 0)))
    arrays, specs = [], []
    for kind, three in enumerate((weights, m, v)):
        for i, a in enumerate(three):
            early = (kind, i) in EARLY
            arrays.append(pltpu.with_memory_space_constraint(a, pltpu.VMEM if early else pltpu.HBM))
            specs.append(at(memory_space=pltpu.VMEM) if early else native[i])
    g = pltpu.with_memory_space_constraint(g, pltpu.HBM)
    return pl.pallas_call(
        update,
        grid=(2, OWNERS),
        in_specs=[at((8, 128), lambda l, o: (0, 0)), *mine, *specs],
        out_specs=native * 3,
        out_shape=[jax.ShapeDtypeStruct(a.shape, a.dtype) for a in arrays],
        compiler_params=pltpu.CompilerParams(vmem_limit_bytes=15 * 2**20),
    )(factor, g, g, g, *arrays)


def solution(mesh, **options):
    def step(x, dy, *arrays):
        weights, m, v = (arrays[i : i + 3] for i in (0, 3, 6))
        state = [weights, m, v]
        g, factor, early = gradients_of(x[0], dy[0], *weights, [state[kind][i] for kind, i in EARLY], **options)
        state = [list(three) for three in state]
        for (kind, i), a in zip(EARLY, early):
            state[kind][i] = a
        return tuple(updated(g.reshape(2, CHUNKS, *g.shape[1:]), factor, *state))

    states, cut = P(("rep", "r", "s"), None, None), P(None, "s", None)
    return jax.shard_map(
        step,
        mesh=mesh,
        in_specs=(states, states) + (cut,) * 9,
        out_specs=(P("rep", "s", None),) * 9,
        check_vma=False,
    )
```

```python
import functools

import jax
import jax.numpy as jnp
from jax import lax
from jax.experimental import pallas as pl
from jax.experimental.pallas import tpu as pltpu
from jax.sharding import PartitionSpec as P

MESH = pl.DeviceIdType.MESH
CHUNKS, CORES, XS, YS, ZS, OWNERS = 8, 2, 2, 2, 4, 4
FIRST = 0
f32, bf16 = jnp.float32, jnp.bfloat16

EARLY = ((1, 0), (1, 1), (1, 2), (2, 0), (2, 1))


def dotn(a, b):
    return jnp.dot(a, b, preferred_element_type=f32)


def dott(a, b):
    return lax.dot_general(a, b, (((1,), (1,)), ((), ())), preferred_element_type=f32)


def dot0(a, b):
    return lax.dot_general(a, b, (((0,), (0,)), ((), ())), preferred_element_type=f32)


def kernel(
    sizes,
    x_hbm, dy_hbm, wg_hbm, wu_hbm, wd_hbm, *refs,
):
    early, refs = refs[: len(EARLY)], refs[len(EARLY) :]
    kernel_(sizes, x_hbm, dy_hbm, wg_hbm, wu_hbm, wd_hbm, early, refs[4 : 4 + len(EARLY)], *refs[:4], *refs[4 + len(EARLY) :])


def kernel_(
    sizes,
    x_hbm, dy_hbm, wg_hbm, wu_hbm, wd_hbm, early, early_out, gfin, factor, wbuf, a0_hbm,
    A, DH, H, total, W, act_s, du_s, dg_s, accs,
    sb0, rb0, own0, sb1, rb1, own1, sb2, rb2, own2, sb3, rb3, own3, piece, squares, over_r, over_s,
    in_sem, early_sem, w_sem, out_sem,
    ws_send, wf_send, w_recv,
    s0, r0, s1, r1, s2, r2, s3, r3, s4, r4, s5, r5, sn, rn, sm, rm,
):
    T, D, F, Tt, rb, cb, LANES = sizes
    COUNT = 2 * CHUNKS * 3 * D * F
    R = D // OWNERS
    HALF, QUARTER = R // YS, R // (YS * ZS)
    nt = T // Tt
    per = nt // 2
    me_r, me_s = lax.axis_index("r"), lax.axis_index("s")
    core, mx = lax.rem(me_s, CORES), me_s // CORES
    my, mz = me_r // ZS, lax.rem(me_r, ZS)
    partner = mx * CORES + 1 - core
    across = (1 - mx) * CORES + core
    to_partner = {"r": me_r, "s": partner}
    to_across = {"r": me_r, "s": across}
    to_y = {"r": (1 - my) * ZS + mz, "s": me_s}

    def remote(src, dst, send, recv, where):
        return pltpu.make_async_remote_copy(src, dst, send, recv, device_id=where, device_id_type=MESH)

    def rows(owner):
        return pl.ds(pl.multiple_of(owner * R, R), R)

    def half(h):
        return pl.ds(pl.multiple_of(h * HALF, HALF), HALF)

    def part_of(owner, h):
        return pl.ds(pl.multiple_of(owner * R + h * HALF, HALF), HALF)

    def own_pieces(l, j, into, h=None):
        wide = F // OWNERS
        there = rows(me_s) if h is None else part_of(me_s, h)
        for m, w in ((0, wg_hbm), (1, wu_hbm)):
            for o in range(OWNERS):
                cols = pl.ds(pl.multiple_of(o * wide * CHUNKS + j * wide, wide), wide)
                src = w.at[l, :, cols] if h is None else w.at[l, half(h), cols]
                yield m, src, into.at[m, there, o * wide : (o + 1) * wide]
        here = rows(j) if h is None else part_of(j, h)
        yield 2, wd_hbm.at[l, here, :], into.at[2, there, :]

    def chunk_of(c):
        return c // CHUNKS, lax.rem(c, CHUNKS)

    def send_own(c):
        l, j = chunk_of(c)
        for m, src, dst in own_pieces(l, j, wbuf.at[l, j], my):
            at = m if c is FIRST else c + 2
            remote(src, dst, ws_send.at[0, c], w_recv.at[0, at], to_across).start()
        for m, src, dst in own_pieces(l, j, wbuf.at[l, j]):
            remote(src, dst, ws_send.at[1, c], w_recv.at[1, c + 2], to_partner).start()

    def pass_on(kind, c, owner, h, where, m=None):
        l, j = chunk_of(c)
        part = wbuf.at[l, j, :, part_of(owner, h), :] if m is None else wbuf.at[l, j, m, part_of(owner, h), :]
        at = c + 2 if m is None else m
        return remote(part, part, wf_send.at[max(kind - 2, 0), at], w_recv.at[kind, at], where)

    def forward(c, m=None):
        pass_on(0, c, across, my, to_across, m).wait_recv()
        pass_on(3, c, across, my, to_y, m).start()
        pass_on(2, c, across, my, to_partner, m).start()

    def forward2(c, m=None):
        pass_on(3, c, across, 1 - my, to_y, m).wait_recv()
        pass_on(4, c, across, 1 - my, to_partner, m).start()

    def load(n):
        slot = lax.rem(n, 2)
        l, j = lax.rem(n // CHUNKS, 2), lax.rem(n, CHUNKS)

        def wait_all(each):
            whole = wbuf.at[l, j, :, rows(partner), :]
            remote(whole, whole, ws_send.at[1, n], w_recv.at[1, n + 2], to_partner).wait_recv()
            for m in each:
                pass_on(2, n, partner, my, to_partner, m).wait_recv()
                pass_on(4, n, partner, 1 - my, to_partner, m).wait_recv()

        if n is FIRST:
            wait_all(range(3))
        else:
            pl.when(n < 2 * CHUNKS)(lambda: wait_all([None]))
        for _, src, dst in own_pieces(l, j, W.at[slot]):
            pltpu.make_async_copy(src, dst, w_sem.at[slot]).start()
        for k in range(1, OWNERS):
            o = lax.rem(me_s + k, OWNERS)
            pltpu.make_async_copy(wbuf.at[l, j, :, rows(o), :], W.at[slot, :, rows(o), :], w_sem.at[slot]).start()

    def wait_load(n):
        slot = lax.rem(n, 2)
        pltpu.make_async_copy(wbuf.at[0, 0], W.at[slot], w_sem.at[slot]).wait()

    def c0(q, m):
        slot = lax.rem(q, 2)
        return remote(sb0.at[m], rb0.at[slot, m], s0.at[m], r0.at[slot, m], to_partner)

    def g0(q, m):
        for xx in range(XS):
            sb0[m, xx] = accs[m, rows(xx * CORES + 1 - core), :].astype(bf16)
        for xx in range(XS):
            own0[m, xx] = accs[m, rows(xx * CORES + core), :]
        c0(q, m).start()

    def c1(q, m):
        slot = lax.rem(q, 2)
        return remote(sb1.at[m], rb1.at[slot, m], s1.at[m], r1.at[slot, m], to_across)

    def g1(q, m):
        c0(q, m).wait()
        slot = lax.rem(q, 2)
        sb1[m] = (own0[m, 1 - mx] + rb0[slot, m, 1 - mx].astype(f32)).astype(bf16)
        own1[m] = own0[m, mx] + rb0[slot, m, mx].astype(f32)
        c1(q, m).start()

    def c2(q, m):
        slot = lax.rem(q, 2)
        return remote(sb2.at[m], rb2.at[slot, m], s2.at[m], r2.at[slot, m], to_y)

    def g2(q, m):
        c1(q, m).wait()
        slot = lax.rem(q, 2)
        sb2[m] = (own1[m, half(1 - my), :] + rb1[slot, m, half(1 - my), :].astype(f32)).astype(bf16)
        own2[m] = own1[m, half(my), :] + rb1[slot, m, half(my), :].astype(f32)
        c2(q, m).start()

    def quarter(z):
        return pl.ds(pl.multiple_of(z * QUARTER, QUARTER), QUARTER)

    def c3(q, m, k):
        where = {"r": my * ZS + lax.rem(mz + 1 + k, ZS), "s": me_s}
        slot = lax.rem(q, 2)
        return remote(sb3.at[m, k], rb3.at[slot, m, k], s3.at[m, k], r3.at[slot, m, k], where)

    def g3(q, m):
        c2(q, m).wait()
        slot = lax.rem(q, 2)
        for k in range(ZS - 1):
            z = lax.rem(mz + 1 + k, ZS)
            sb3[m, k] = (own2[m, quarter(z), :] + rb2[slot, m, quarter(z), :].astype(f32)).astype(bf16)
        own3[m] = own2[m, quarter(mz), :] + rb2[slot, m, quarter(mz), :].astype(f32)
        for k in range(ZS - 1):
            c3(q, m, k).start()

    mine = pl.ds(pl.multiple_of(my * HALF + mz * QUARTER, QUARTER), QUARTER)

    def to_peer(k):
        return {"r": lax.rem(me_r + 1 + k, YS * ZS), "s": me_s}

    def c4(q, m, k):
        where = {"r": my * ZS + lax.rem(mz + 1 + k, ZS), "s": me_s}
        return remote(piece.at[q, m], gfin.at[q, m, mine, :], s4.at[lax.rem(q, 2), m], r4.at[lax.rem(q, 2), m], where)

    def c4_here(q, m):
        return pltpu.make_async_copy(piece.at[q, m], gfin.at[q, m, mine, :], out_sem.at[lax.rem(q, 2), m])

    def g4(q, m):
        slot = lax.rem(q, 2)
        for k in range(ZS - 1):
            c3(q, m, k).wait()
        v = own3[m]
        for k in range(ZS - 1):
            v += rb3[slot, m, k].astype(f32)
        v = v.astype(bf16)
        piece[q, m] = v
        v = v.astype(f32)
        squares[...] += sum(v[:, i : i + LANES] * v[:, i : i + LANES] for i in range(0, F, LANES))
        for k in range(ZS - 1):
            c4(q, m, k).start()
        c4_here(q, m).start()

    def c5(q, m):
        part = gfin.at[q, m, half(my), :]
        return remote(part, part, s5.at[lax.rem(q, 2), m], r5.at[lax.rem(q, 2), m], to_y)

    def g5(q, m):
        others = gfin.at[q, m, : HALF - QUARTER, :]
        remote(others, others, s4.at[lax.rem(q, 2), m], r4.at[lax.rem(q, 2), m], to_y).wait()
        c4_here(q, m).wait()
        c5(q, m).start()

    def g6(q, m):
        c5(q, m).wait()

    def each(stage, which=(0, 1, 2)):
        def run(q):
            for m in which:
                stage(q, m)

        run.__name__ = stage.__name__
        return run

    def when(test, what, q):
        def run():
            with jax.named_scope(what.__name__):
                what(q)
        pl.when(test)(run)

    last = 2 * CHUNKS

    def exchange(q, b):
        def at(stage, *parts):
            @pl.when(b == stage)
            def _():
                for back, what, which in parts:
                    when(q >= back, each(what, which), q - back)

        every = (0, 1, 2)
        at(0, (2, g2, (2,)), (1, g0, every), (3, g4, (2,)), (4, g6, every))
        at(1, (1, g1, every), (2, g3, (0, 1)), (3, g5, (0, 1)))
        at(2, (2, g3, (2,)), (3, g5, (2,)))
        at(3, (1, g2, (0, 1)), (2, g4, (0, 1)))

    def drain():
        a, b, c = last - 3, last - 2, last - 1
        each(g0)(c)
        g2(b, 2)
        each(g6)(a - 1)
        g4(a, 2)
        each(g3, (0, 1))(b)
        each(g1)(c)
        each(g5, (0, 1))(a)
        g3(b, 2)
        each(g4, (0, 1))(b)
        g5(a, 2)
        g2(c, 0)
        g4(b, 2)
        each(g6)(a)
        g2(c, 1)
        g3(c, 0)
        each(g5, (0, 1))(b)
        g2(c, 2)
        g3(c, 1)
        g5(b, 2)
        g4(c, 0)
        g3(c, 2)
        g4(c, 1)
        each(g6)(b)
        g5(c, 0)
        g4(c, 2)
        over_r[me_r] = squares[...]
        peers_r = [to_peer(k) for k in range(YS * ZS - 1)]
        from_r = [lax.rem(me_r + YS * ZS - 1 - k, YS * ZS) for k in range(YS * ZS - 1)]
        peers_s = [{"r": me_r, "s": lax.rem(me_s + 1 + k, OWNERS)} for k in range(OWNERS - 1)]
        from_s = [lax.rem(me_s + OWNERS - 1 - k, OWNERS) for k in range(OWNERS - 1)]
        tell(me_r, over_r, sn, rn, peers_r)
        g5(c, 1)
        hear(me_r, over_r, sn, rn, peers_r, from_r)
        over_s[me_s] = jnp.sum(over_r[...], 0)
        tell(me_s, over_s, sm, rm, peers_s)
        g5(c, 2)
        hear(me_s, over_s, sm, rm, peers_s, from_s)
        each(g6)(c)

    def tell(me, scratch, send, recv, others):
        for k, where in enumerate(others):
            remote(scratch.at[me], scratch.at[me], send.at[k], recv.at[k], where).start()

    def hear(me, scratch, send, recv, others, places):
        for k, (where, place) in enumerate(zip(others, places)):
            remote(scratch.at[me], scratch.at[place], send.at[k], recv.at[k], where).wait()

    def normed(wide):
        scale = lax.rsqrt(jnp.mean(wide * wide, -1, keepdims=True) + 1e-6)
        return (wide * scale).astype(bf16)

    def tile(t, n=Tt):
        return pl.ds(pl.multiple_of(t * n, n), n)

    def first(wslot, t, slot, backward, r, c):
        s = pl.ds(pl.multiple_of(t * Tt + r * rb, rb), rb)
        rs, cs = slice(r * rb, (r + 1) * rb), slice(c * cb, (c + 1) * cb)
        a = A[s, :]
        g = dotn(a, W[wslot, 0, :, cs])
        u = dotn(a, W[wslot, 1, :, cs])
        h = 0.5 * g
        th = jnp.tanh(h)
        silu = h * th + h
        if not backward:
            act_s[slot, rs, cs] = (silu * u).astype(bf16)
            return
        d = dott(DH[s, :], W[wslot, 2, cs, :]).astype(bf16).astype(f32)
        sig = 0.5 * th + 0.5
        act_s[slot, rs, cs] = (silu * u).astype(bf16)
        du_s[slot, rs, cs] = (d * silu).astype(bf16)
        dg_s[slot, rs, cs] = (d * u * (sig * (1.0 + g - silu))).astype(bf16)

    def second(wslot, t, slot, backward, input_too, begin, which):
        s = tile(t)
        if not backward:
            total[s, :] += dotn(act_s[slot], W[wslot, 2])
            return
        if which == 3:
            total[s, :] += dott(dg_s[slot], W[wslot, 0]) + dott(du_s[slot], W[wslot, 1])
            return
        if which == 2:
            new = dot0(act_s[slot], DH[s, :])
        else:
            new = dot0(A[s, :], (dg_s, du_s)[which][slot])
        if begin:
            accs[which] = jnp.where(t == 0, 0.0, accs[which]) + new
        else:
            accs[which] += new

    blocks = [(r, c) for r in range(Tt // rb) for c in range(F // cb)]

    def together(w1, t1, slot1, w2, t2, slot2, backward, input_too, begin):
        for which in range(4 if input_too else 3) if backward else [0]:
            second(w2, t2, slot2, backward, input_too, begin, which)
        for block in blocks:
            first(w1, t1, slot1, backward, *block)

    def phase(base, backward, input_too):
        for block in blocks:
            first(lax.rem(base, 2), 0, 0, backward, *block)

        def step(i, _):
            n, b = base + i // per, lax.rem(i, per)
            if backward:
                exchange(n - CHUNKS, b)
            if base < 2 * CHUNKS:

                @pl.when(b == 0)
                def _():
                    when(n + 4 < 2 * CHUNKS, send_own, n + 4)

                @pl.when(b == 1)
                def _():
                    when(n + 1 < 2 * CHUNKS, forward2, n + 1)
                    when(n + 2 < 2 * CHUNKS, forward, n + 2)

            when((b == 2) & (n + 1 < 3 * CHUNKS), load, n + 1)
            when((b == per - 1) & (n + 1 < 3 * CHUNKS), wait_load, n + 1)
            w = lax.rem(n, 2)
            t = 2 * b
            together(w, t + 1, 1, w, t, 0, backward, input_too, True)
            over = b == per - 1
            together(jnp.where(over, 1 - w, w), jnp.where(over, 0, t + 2), 0, w, t + 1, 1, backward, input_too, False)
            return 0

        lax.fori_loop(0, per * CHUNKS, step, 0)

    barrier = pltpu.get_barrier_semaphore()
    peers = [to_partner, to_across] + [{"r": lax.rem(me_r + k, YS * ZS), "s": me_s} for k in range(1, YS * ZS)]
    for peer in peers:
        pl.semaphore_signal(barrier, inc=1, device_id=peer, device_id_type=MESH)
    load_x = pltpu.make_async_copy(x_hbm, H, in_sem.at[0])
    load_dy = pltpu.make_async_copy(dy_hbm, DH, in_sem.at[1])
    load_x.start()
    load_dy.start()
    with jax.named_scope('barrier'):
        pl.semaphore_wait(barrier, len(peers))
    send_own(FIRST)
    lax.fori_loop(1, 4, lambda c, _: (send_own(c), 0)[1], 0)
    load_x.wait()

    def begin(t, _):
        s = tile(t, rb)
        A[s, :] = normed(H[s, :].astype(f32))
        total[s, :] = jnp.zeros((rb, D), f32)
        return 0

    squares[...] = jnp.zeros(squares.shape, f32)
    with jax.named_scope('begin'):
        lax.fori_loop(0, T // rb, begin, 0)
    save_a = pltpu.make_async_copy(A, a0_hbm, in_sem.at[0])
    save_a.start()
    with jax.named_scope('first_load'):
        for m in range(3):
            forward(FIRST, m)
        for m in range(3):
            forward2(FIRST, m)
        load(FIRST)
        forward(1)
        wait_load(0)
    with jax.named_scope('p_fwd'):
        phase(0, False, False)
    save_a.wait()
    load_dy.wait()

    def between(t, _):
        s = tile(t, rb)
        h = (H[s, :].astype(f32) + total[s, :].astype(bf16).astype(f32)).astype(bf16)
        H[s, :] = h
        A[s, :] = normed(h.astype(f32))
        total[s, :] = jnp.zeros((rb, D), f32)
        return 0

    with jax.named_scope('between'):
        lax.fori_loop(0, T // rb, between, 0)
    with jax.named_scope('p_one'):
        phase(CHUNKS, True, True)
    load_a = pltpu.make_async_copy(a0_hbm, A, in_sem.at[0])
    load_a.start()

    def back(t, _):
        s = tile(t, rb)
        wide = H[s, :].astype(f32)
        da = total[s, :].astype(bf16).astype(f32)
        scale = lax.rsqrt(jnp.mean(wide * wide, -1, keepdims=True) + 1e-6)
        along = jnp.sum(da * wide, -1, keepdims=True) * (scale * scale * scale * (1.0 / D))
        dn = (da * scale - wide * along).astype(bf16).astype(f32)
        DH[s, :] = (DH[s, :].astype(f32) + dn).astype(bf16)
        return 0

    with jax.named_scope('back'):
        lax.fori_loop(0, T // rb, back, 0)
        load_a.wait()
    fetch = [pltpu.make_async_copy(src, dst, early_sem.at[i]) for i, (src, dst) in enumerate(zip(early, early_out))]
    for copy in fetch:
        copy.start()
    with jax.named_scope('p_zero'):
        phase(2 * CHUNKS, True, False)

    with jax.named_scope("drain"):
        drain()
    with jax.named_scope("norm"):
        mean = jnp.sum(over_s[...]) * (1.0 / COUNT)
        factor[...] = jnp.minimum(1.0, 0.5 * lax.rsqrt(jnp.full(factor.shape, mean + 1e-30, f32)))

    def finish(q, _):
        l, j = q // CHUNKS, lax.rem(q, CHUNKS)
        one = wbuf.at[l, j, :, :R, :]
        remote(one, one, ws_send.at[1, q], w_recv.at[1, q + 2], to_partner).wait_send()
        one = wbuf.at[l, j, :, :HALF, :]
        remote(one, one, ws_send.at[0, q], w_recv.at[0, q + 2], to_across).wait_send()

        def passed(each):
            for m in each:
                for kind in (2, 3, 4):
                    pass_on(kind, q, across, my, to_partner, m).wait_send()

        pl.when(q == 0)(lambda: passed(range(3)))
        pl.when(q > 0)(lambda: passed([None]))
        return 0

    for copy in fetch:
        copy.wait()
    with jax.named_scope('finish'):
        lax.fori_loop(0, last, finish, 0)


def gradients_of(x, dy, w_gate, w_up, w_down, early, tiles=(512, 256, 256), vmem=41 * 2**20):
    T, D = x.shape
    F = w_gate.shape[2] // CHUNKS
    Tt, rb, cb = tiles
    R = D // OWNERS
    H, Q = R // YS, R // (YS * ZS)
    n = 2 * CHUNKS
    lanes = min(F, 128)
    vm = pltpu.VMEM
    dma, hbm = pltpu.SemaphoreType.DMA, pl.BlockSpec(memory_space=pltpu.HBM)
    outs = pl.pallas_call(
        functools.partial(kernel, (T, D, F, Tt, rb, cb, lanes)),
        in_specs=[hbm] * (5 + len(early)),
        out_specs=[hbm, pl.BlockSpec(memory_space=pltpu.VMEM), hbm, hbm] + [pl.BlockSpec(memory_space=pltpu.VMEM)] * len(early),
        out_shape=[
            pltpu.HBM((n, 3, R, F), bf16), pltpu.VMEM((8, 128), f32),
            pltpu.HBM((2, CHUNKS, 3, D, F), bf16), pltpu.HBM((T, D), bf16),
            *(pltpu.VMEM(a.shape, a.dtype) for a in early),
        ],
        scratch_shapes=[
            vm((T, D), bf16), vm((T, D), bf16), vm((T, D), bf16), vm((T, D), f32),
            vm((2, 3, D, F), bf16), vm((2, Tt, F), bf16), vm((2, Tt, F), bf16), vm((2, Tt, F), bf16), vm((3, D, F), f32),
            vm((3, XS, R, F), bf16), vm((2, 3, XS, R, F), bf16), vm((3, XS, R, F), f32),
            vm((3, R, F), bf16), vm((2, 3, R, F), bf16), vm((3, R, F), f32),
            vm((3, H, F), bf16), vm((2, 3, H, F), bf16), vm((3, H, F), f32),
            vm((3, ZS - 1, Q, F), bf16), vm((2, 3, ZS - 1, Q, F), bf16), vm((3, Q, F), f32),
            vm((n, 3, Q, F), bf16), vm((Q, lanes), f32), vm((YS * ZS, Q, lanes), f32), vm((OWNERS, Q, lanes), f32),
            dma((2,)), dma((len(early),)), dma((2,)), dma((2, 3)),
            dma((2, n)), dma((3, n + 2)), dma((5, n + 2)),
            dma((3,)), dma((2, 3)), dma((3,)), dma((2, 3)), dma((3,)), dma((2, 3)), dma((3, ZS - 1)), dma((2, 3, ZS - 1)), dma((2, 3)), dma((2, 3)), dma((2, 3)), dma((2, 3)),
            dma((YS * ZS - 1,)), dma((YS * ZS - 1,)), dma((OWNERS - 1,)), dma((OWNERS - 1,)),
        ],
        compiler_params=pltpu.CompilerParams(collective_id=0, has_side_effects=True, vmem_limit_bytes=vmem),
    )(*(pltpu.with_memory_space_constraint(a, pltpu.HBM) for a in (x, dy, w_gate, w_up, w_down, *early)))
    return outs[0], outs[1], outs[4:]


def update(factor, ga, gb, gc, *refs):
    l, o = pl.program_id(0), pl.program_id(1)
    scale = factor[0:1, 0:1]
    for i, g in enumerate((ga, gb, gc)):
        _, parts, _, R, wide = g.shape
        size = wide if i < 2 else R
        for j in range(parts):
            near = slice(j * size, (j + 1) * size)
            far = pl.ds(pl.multiple_of((o * parts + j) * size, size), size)

            def read(kind):
                ref, layer, cut = (refs[3 * kind + i], l, far) if (kind, i) in EARLY else (refs[3 * kind + i], 0, near)
                return ref[layer, :, cut] if i < 2 else ref[layer, cut, :]

            def write(kind, value):
                if i < 2:
                    refs[9 + 3 * kind + i][0, :, near] = value
                else:
                    refs[9 + 3 * kind + i][0, near, :] = value

            gradient = g[0, j, 0].astype(f32) * scale
            m = 0.9 * read(1) + 0.1 * gradient
            v = 0.95 * read(2) + 0.05 * gradient * gradient
            w = read(0).astype(f32)
            write(0, (w - 0.02 * (m * lax.rsqrt(v + 1e-8) + 0.1 * w)).astype(bf16))
            write(1, m)
            write(2, v)


def updated(g, factor, weights, m, v):
    _, _, _, R, F = g.shape
    wide = F // OWNERS
    at = pl.BlockSpec
    native = [at((1, R, CHUNKS * wide), lambda l, o: (l, 0, o))] * 2 + [at((1, CHUNKS * R // OWNERS, F), lambda l, o: (l, o, 0))]
    mine = [at((1, CHUNKS, 1, R, wide), lambda l, o, k=k: (1 - l, 0, k, 0, o)) for k in range(2)]
    mine.append(at((1, CHUNKS // OWNERS, 1, R, F), lambda l, o: (1 - l, o, 2, 0, 0)))
    arrays, specs = [], []
    for kind, three in enumerate((weights, m, v)):
        for i, a in enumerate(three):
            early = (kind, i) in EARLY
            arrays.append(pltpu.with_memory_space_constraint(a, pltpu.VMEM if early else pltpu.HBM))
            specs.append(at(memory_space=pltpu.VMEM) if early else native[i])
    g = pltpu.with_memory_space_constraint(g, pltpu.HBM)
    return pl.pallas_call(
        update,
        grid=(2, OWNERS),
        in_specs=[at((8, 128), lambda l, o: (0, 0)), *mine, *specs],
        out_specs=native * 3,
        out_shape=[jax.ShapeDtypeStruct(a.shape, a.dtype) for a in arrays],
        compiler_params=pltpu.CompilerParams(vmem_limit_bytes=15 * 2**20),
    )(factor, g, g, g, *arrays)


def solution(mesh, **options):
    def step(x, dy, *arrays):
        weights, m, v = (arrays[i : i + 3] for i in (0, 3, 6))
        state = [weights, m, v]
        g, factor, early = gradients_of(x[0], dy[0], *weights, [state[kind][i] for kind, i in EARLY], **options)
        state = [list(three) for three in state]
        for (kind, i), a in zip(EARLY, early):
            state[kind][i] = a
        return tuple(updated(g.reshape(2, CHUNKS, *g.shape[1:]), factor, *state))

    states, cut = P(("rep", "r", "s"), None, None), P(None, "s", None)
    return jax.shard_map(
        step,
        mesh=mesh,
        in_specs=(states, states) + (cut,) * 9,
        out_specs=(P("rep", "s", None),) * 9,
        check_vma=False,
    )
```

```python
import functools

import jax
import jax.numpy as jnp
from jax import lax
from jax.experimental import pallas as pl
from jax.experimental.pallas import tpu as pltpu
from jax.sharding import PartitionSpec as P

MESH = pl.DeviceIdType.MESH
CHUNKS, CORES, XS, YS, ZS, OWNERS = 8, 2, 2, 2, 4, 4
FIRST = 0
f32, bf16 = jnp.float32, jnp.bfloat16

def dotn(a, b):
    return jnp.dot(a, b, preferred_element_type=f32)


def dott(a, b):
    return lax.dot_general(a, b, (((1,), (1,)), ((), ())), preferred_element_type=f32)


def dot0(a, b):
    return lax.dot_general(a, b, (((0,), (0,)), ((), ())), preferred_element_type=f32)


def kernel(
    sizes,
    x_hbm, dy_hbm, wg_hbm, wu_hbm, wd_hbm, *refs,
):
    early, refs = refs[:5], refs[5:]
    kernel_(sizes, x_hbm, dy_hbm, wg_hbm, wu_hbm, wd_hbm, early, refs[4:9], *refs[:4], *refs[9:])


def kernel_(
    sizes,
    x_hbm, dy_hbm, wg_hbm, wu_hbm, wd_hbm, early, early_out, gfin, factor, wbuf, a0_hbm,
    H, A, DH, total, W, act_s, du_s, dg_s, accs,
    sb0, rb0, own0, sb1, rb1, own1, sb2, rb2, own2, sb3, rb3, own3, piece, squares, over_r, over_s,
    in_sem, early_sem, w_sem, keep_sem, out_sem,
    ws_send, wf_send, w_recv,
    s0, r0, s1, r1, s2, r2, s3, r3, s4, r4, s5, r5, sn, rn, sm, rm,
):
    T, D, F, Tt, rb, cb, LANES = sizes
    COUNT = 2 * CHUNKS * 3 * D * F
    R = D // OWNERS
    HALF, QUARTER = R // YS, R // (YS * ZS)
    nt = T // Tt
    per = nt // 2
    me_r, me_s = lax.axis_index("r"), lax.axis_index("s")
    core, mx = lax.rem(me_s, CORES), me_s // CORES
    my, mz = me_r // ZS, lax.rem(me_r, ZS)
    partner = mx * CORES + 1 - core
    across = (1 - mx) * CORES + core
    to_partner = {"r": me_r, "s": partner}
    to_across = {"r": me_r, "s": across}
    to_y = {"r": (1 - my) * ZS + mz, "s": me_s}

    def remote(src, dst, send, recv, where):
        return pltpu.make_async_remote_copy(src, dst, send, recv, device_id=where, device_id_type=MESH)

    def rows(owner):
        return pl.ds(pl.multiple_of(owner * R, R), R)

    def half(h):
        return pl.ds(pl.multiple_of(h * HALF, HALF), HALF)

    def part_of(owner, h):
        return pl.ds(pl.multiple_of(owner * R + h * HALF, HALF), HALF)

    def own_pieces(l, j, into, h=None):
        wide = F // OWNERS
        there = rows(me_s) if h is None else part_of(me_s, h)
        for m, w in ((0, wg_hbm), (1, wu_hbm)):
            for o in range(OWNERS):
                cols = pl.ds(pl.multiple_of(o * wide * CHUNKS + j * wide, wide), wide)
                src = w.at[l, :, cols] if h is None else w.at[l, half(h), cols]
                yield m, src, into.at[m, there, o * wide : (o + 1) * wide]
        here = rows(j) if h is None else part_of(j, h)
        yield 2, wd_hbm.at[l, here, :], into.at[2, there, :]

    def chunk_of(c):
        return c // CHUNKS, lax.rem(c, CHUNKS)

    def send_own(c):
        l, j = chunk_of(c)
        into = W.at[0] if c is FIRST else wbuf.at[l, j]
        for m, src, dst in own_pieces(l, j, into, my):
            at = m if c is FIRST else c + 2
            remote(src, dst, ws_send.at[0, c], w_recv.at[0, at], to_across).start()
        for m, src, dst in own_pieces(l, j, into):
            remote(src, dst, ws_send.at[1, c], w_recv.at[1, c + 2], to_partner).start()

    def pass_on(kind, c, owner, h, where, m=None):
        l, j = chunk_of(c)
        part = wbuf.at[l, j, :, part_of(owner, h), :] if m is None else W.at[0, m, part_of(owner, h), :]
        at = c + 2 if m is None else m
        return remote(part, part, wf_send.at[max(kind - 2, 0), at], w_recv.at[kind, at], where)

    def forward(c, m=None):
        pass_on(0, c, across, my, to_across, m).wait_recv()
        pass_on(3, c, across, my, to_y, m).start()
        pass_on(2, c, across, my, to_partner, m).start()

    def forward2(c, m=None):
        pass_on(3, c, across, 1 - my, to_y, m).wait_recv()
        pass_on(4, c, across, 1 - my, to_partner, m).start()

    def load(n):
        slot = lax.rem(n, 2)
        l, j = lax.rem(n // CHUNKS, 2), lax.rem(n, CHUNKS)

        @pl.when(n < 2 * CHUNKS)
        def _():
            whole = wbuf.at[l, j, :, rows(partner), :]
            remote(whole, whole, ws_send.at[1, n], w_recv.at[1, n + 2], to_partner).wait_recv()
            pass_on(2, n, partner, my, to_partner).wait_recv()
            pass_on(4, n, partner, 1 - my, to_partner).wait_recv()

        for _, src, dst in own_pieces(l, j, W.at[slot]):
            pltpu.make_async_copy(src, dst, w_sem.at[slot]).start()
        for k in range(1, OWNERS):
            o = lax.rem(me_s + k, OWNERS)
            pltpu.make_async_copy(wbuf.at[l, j, :, rows(o), :], W.at[slot, :, rows(o), :], w_sem.at[slot]).start()

    def load_first():
        for _, src, dst in own_pieces(0, 0, W.at[0]):
            pltpu.make_async_copy(src, dst, w_sem.at[0]).start()

    def wait_first():
        mine = W.at[0, :, rows(me_s), :]
        pltpu.make_async_copy(mine, mine, w_sem.at[0]).wait()
        whole = W.at[0, :, rows(partner), :]
        remote(whole, whole, ws_send.at[1, 0], w_recv.at[1, 2], to_partner).wait_recv()
        for m in range(3):
            pass_on(2, FIRST, partner, my, to_partner, m).wait_recv()
            pass_on(4, FIRST, partner, 1 - my, to_partner, m).wait_recv()

    def keep_first():
        return pltpu.make_async_copy(W.at[0], wbuf.at[0, 0], keep_sem)

    def free_first(_):
        keep_first().wait()
        for m in range(3):
            for kind in (2, 3, 4):
                pass_on(kind, FIRST, across, my, to_partner, m).wait_send()

    def wait_load(n):
        slot = lax.rem(n, 2)
        pltpu.make_async_copy(wbuf.at[0, 0], W.at[slot], w_sem.at[slot]).wait()

    def c0(q, m):
        slot = lax.rem(q, 2)
        return remote(sb0.at[m], rb0.at[slot, m], s0.at[m], r0.at[slot, m], to_partner)

    def g0(q, m):
        for xx in range(XS):
            sb0[m, xx] = accs[m, rows(xx * CORES + 1 - core), :].astype(bf16)
        for xx in range(XS):
            own0[m, xx] = accs[m, rows(xx * CORES + core), :]
        c0(q, m).start()

    def c1(q, m):
        slot = lax.rem(q, 2)
        return remote(sb1.at[m], rb1.at[slot, m], s1.at[m], r1.at[slot, m], to_across)

    def g1(q, m):
        c0(q, m).wait()
        slot = lax.rem(q, 2)
        sb1[m] = (own0[m, 1 - mx] + rb0[slot, m, 1 - mx].astype(f32)).astype(bf16)
        own1[m] = own0[m, mx] + rb0[slot, m, mx].astype(f32)
        c1(q, m).start()

    def c2(q, m):
        slot = lax.rem(q, 2)
        return remote(sb2.at[m], rb2.at[slot, m], s2.at[m], r2.at[slot, m], to_y)

    def g2(q, m):
        c1(q, m).wait()
        slot = lax.rem(q, 2)
        sb2[m] = (own1[m, half(1 - my), :] + rb1[slot, m, half(1 - my), :].astype(f32)).astype(bf16)
        own2[m] = own1[m, half(my), :] + rb1[slot, m, half(my), :].astype(f32)
        c2(q, m).start()

    def quarter(z):
        return pl.ds(pl.multiple_of(z * QUARTER, QUARTER), QUARTER)

    def c3(q, m, k):
        where = {"r": my * ZS + lax.rem(mz + 1 + k, ZS), "s": me_s}
        slot = lax.rem(q, 2)
        return remote(sb3.at[m, k], rb3.at[slot, m, k], s3.at[m, k], r3.at[slot, m, k], where)

    def g3(q, m):
        c2(q, m).wait()
        slot = lax.rem(q, 2)
        for k in range(ZS - 1):
            z = lax.rem(mz + 1 + k, ZS)
            sb3[m, k] = (own2[m, quarter(z), :] + rb2[slot, m, quarter(z), :].astype(f32)).astype(bf16)
        own3[m] = own2[m, quarter(mz), :] + rb2[slot, m, quarter(mz), :].astype(f32)
        for k in range(ZS - 1):
            c3(q, m, k).start()

    mine = pl.ds(pl.multiple_of(my * HALF + mz * QUARTER, QUARTER), QUARTER)

    def to_peer(k):
        return {"r": lax.rem(me_r + 1 + k, YS * ZS), "s": me_s}

    def c4(q, m, k):
        where = {"r": my * ZS + lax.rem(mz + 1 + k, ZS), "s": me_s}
        return remote(piece.at[q, m], gfin.at[q, m, mine, :], s4.at[lax.rem(q, 2), m], r4.at[lax.rem(q, 2), m], where)

    def c4_here(q, m):
        return pltpu.make_async_copy(piece.at[q, m], gfin.at[q, m, mine, :], out_sem.at[lax.rem(q, 2), m])

    def g4(q, m, then=None):
        slot = lax.rem(q, 2)
        for k in range(ZS - 1):
            c3(q, m, k).wait()
        v = own3[m]
        for k in range(ZS - 1):
            v += rb3[slot, m, k].astype(f32)
        v = v.astype(bf16)
        piece[q, m] = v
        v = v.astype(f32)
        squares[...] += sum(v[:, i : i + LANES] * v[:, i : i + LANES] for i in range(0, F, LANES))
        if then is not None:
            then()
        for k in range(ZS - 1):
            c4(q, m, k).start()
        c4_here(q, m).start()

    def c5(q, m):
        part = gfin.at[q, m, half(my), :]
        return remote(part, part, s5.at[lax.rem(q, 2), m], r5.at[lax.rem(q, 2), m], to_y)

    def g5(q, m):
        others = gfin.at[q, m, : HALF - QUARTER, :]
        remote(others, others, s4.at[lax.rem(q, 2), m], r4.at[lax.rem(q, 2), m], to_y).wait()
        c4_here(q, m).wait()
        c5(q, m).start()

    def g6(q, m):
        c5(q, m).wait()

    def each(stage, which=(0, 1, 2)):
        def run(q):
            for m in which:
                stage(q, m)

        run.__name__ = stage.__name__
        return run

    def when(test, what, q):
        def run():
            with jax.named_scope(what.__name__):
                what(q)
        pl.when(test)(run)

    last = 2 * CHUNKS

    def exchange(q, b):
        def at(stage, *parts):
            @pl.when(b == stage)
            def _():
                for back, what, which in parts:
                    when(q >= back, each(what, which), q - back)

        every = (0, 1, 2)
        at(0, (2, g2, (2,)), (1, g0, every), (3, g4, (2,)), (4, g6, every))
        at(1, (1, g1, every), (2, g3, (0, 1)), (3, g5, (0, 1)))
        at(2, (2, g3, (2,)), (3, g5, (2,)))
        at(3, (1, g2, (0, 1)), (2, g4, (0, 1)))

    def drain():
        a, b, c = last - 3, last - 2, last - 1
        each(g0)(c)
        g2(b, 2)
        each(g6)(a - 1)
        g4(a, 2)
        each(g3, (0, 1))(b)
        each(g1)(c)
        each(g5, (0, 1))(a)
        g3(b, 2)
        each(g4, (0, 1))(b)
        g5(a, 2)
        g2(c, 0)
        g4(b, 2)
        each(g6)(a)
        g2(c, 1)
        g3(c, 0)
        each(g5, (0, 1))(b)
        g2(c, 2)
        g3(c, 1)
        g5(b, 2)
        g4(c, 0)
        g3(c, 2)
        g4(c, 1)
        each(g6)(b)
        g5(c, 0)
        peers_r = [to_peer(k) for k in range(YS * ZS - 1)]
        from_r = [lax.rem(me_r + YS * ZS - 1 - k, YS * ZS) for k in range(YS * ZS - 1)]
        peers_s = [{"r": me_r, "s": lax.rem(me_s + 1 + k, OWNERS)} for k in range(OWNERS - 1)]
        from_s = [lax.rem(me_s + OWNERS - 1 - k, OWNERS) for k in range(OWNERS - 1)]

        def tell_squares():
            over_r[me_r] = squares[...]
            tell(me_r, over_r, sn, rn, peers_r)

        g4(c, 2, tell_squares)
        g5(c, 1)
        hear(me_r, over_r, sn, rn, peers_r, from_r)
        over_s[me_s] = jnp.sum(over_r[...], 0)
        tell(me_s, over_s, sm, rm, peers_s)
        g5(c, 2)
        hear(me_s, over_s, sm, rm, peers_s, from_s)
        each(g6)(c)

    def tell(me, scratch, send, recv, others):
        for k, where in enumerate(others):
            remote(scratch.at[me], scratch.at[me], send.at[k], recv.at[k], where).start()

    def hear(me, scratch, send, recv, others, places):
        for k, (where, place) in enumerate(zip(others, places)):
            remote(scratch.at[me], scratch.at[place], send.at[k], recv.at[k], where).wait()

    def normed(wide):
        scale = lax.rsqrt(jnp.mean(wide * wide, -1, keepdims=True) + 1e-6)
        return (wide * scale).astype(bf16)

    def tile(t, n=Tt):
        return pl.ds(pl.multiple_of(t * n, n), n)

    def first(wslot, t, slot, backward, r, c):
        s = pl.ds(pl.multiple_of(t * Tt + r * rb, rb), rb)
        rs, cs = slice(r * rb, (r + 1) * rb), slice(c * cb, (c + 1) * cb)
        a = A[s, :]
        g = dotn(a, W[wslot, 0, :, cs])
        u = dotn(a, W[wslot, 1, :, cs])
        h = 0.5 * g
        th = jnp.tanh(h)
        silu = h * th + h
        if not backward:
            act_s[slot, rs, cs] = (silu * u).astype(bf16)
            return
        d = dott(DH[s, :], W[wslot, 2, cs, :]).astype(bf16).astype(f32)
        sig = 0.5 * th + 0.5
        act_s[slot, rs, cs] = (silu * u).astype(bf16)
        du_s[slot, rs, cs] = (d * silu).astype(bf16)
        dg_s[slot, rs, cs] = (d * u * (sig * (1.0 + g - silu))).astype(bf16)

    def second(wslot, t, slot, backward, input_too, begin, which):
        s = tile(t)
        if not backward:
            total[s, :] += dotn(act_s[slot], W[wslot, 2])
            return
        if which == 3:
            total[s, :] += dott(dg_s[slot], W[wslot, 0]) + dott(du_s[slot], W[wslot, 1])
            return
        if which == 2:
            new = dot0(act_s[slot], DH[s, :])
        else:
            new = dot0(A[s, :], (dg_s, du_s)[which][slot])
        if begin:
            accs[which] = jnp.where(t == 0, 0.0, accs[which]) + new
        else:
            accs[which] += new

    blocks = [(r, c) for r in range(Tt // rb) for c in range(F // cb)]

    def together(w1, t1, slot1, w2, t2, slot2, backward, input_too, begin):
        for which in range(4 if input_too else 3) if backward else [0]:
            second(w2, t2, slot2, backward, input_too, begin, which)
        for block in blocks:
            first(w1, t1, slot1, backward, *block)

    def phase(base, backward, input_too):
        for block in blocks:
            first(lax.rem(base, 2), 0, 0, backward, *block)

        def step(i, _):
            n, b = base + i // per, lax.rem(i, per)
            if backward:
                exchange(n - CHUNKS, b)
            if base < 2 * CHUNKS:

                @pl.when(b == 0)
                def _():
                    when(n + 4 < 2 * CHUNKS, send_own, n + 4)

                @pl.when(b == 1)
                def _():
                    when(n + 1 < 2 * CHUNKS, forward2, n + 1)
                    when(n + 2 < 2 * CHUNKS, forward, n + 2)
                    when(n == 1, free_first, n)

            when((b == 2) & (n + 1 < 3 * CHUNKS), load, n + 1)
            when((b == per - 1) & (n + 1 < 3 * CHUNKS), wait_load, n + 1)
            w = lax.rem(n, 2)
            t = 2 * b
            together(w, t + 1, 1, w, t, 0, backward, input_too, True)
            over = b == per - 1
            together(jnp.where(over, 1 - w, w), jnp.where(over, 0, t + 2), 0, w, t + 1, 1, backward, input_too, False)
            return 0

        lax.fori_loop(0, per * CHUNKS, step, 0)

    barrier = pltpu.get_barrier_semaphore()
    peers = [to_partner, to_across] + [{"r": lax.rem(me_r + k, YS * ZS), "s": me_s} for k in range(1, YS * ZS)]
    for peer in peers:
        pl.semaphore_signal(barrier, inc=1, device_id=peer, device_id_type=MESH)
    load_x = pltpu.make_async_copy(x_hbm, H, in_sem.at[0])
    load_dy = pltpu.make_async_copy(dy_hbm, DH, in_sem.at[1])
    load_x.start()
    load_dy.start()
    with jax.named_scope('barrier'):
        pl.semaphore_wait(barrier, len(peers))
    send_own(FIRST)
    load_first()
    lax.fori_loop(1, 4, lambda c, _: (send_own(c), 0)[1], 0)
    load_x.wait()

    def begin(t, _):
        s = tile(t, rb)
        A[s, :] = normed(H[s, :].astype(f32))
        total[s, :] = jnp.zeros((rb, D), f32)
        return 0

    squares[...] = jnp.zeros(squares.shape, f32)
    with jax.named_scope('begin'):
        lax.fori_loop(0, T // rb, begin, 0)
    save_a = pltpu.make_async_copy(A, a0_hbm, in_sem.at[0])
    save_a.start()
    with jax.named_scope('first_load'):
        for m in range(3):
            forward(FIRST, m)
        for m in range(3):
            forward2(FIRST, m)
        forward(1)
        wait_first()
        keep_first().start()
    with jax.named_scope('p_fwd'):
        phase(0, False, False)
    save_a.wait()
    load_dy.wait()

    def between(t, _):
        s = tile(t, rb)
        h = (H[s, :].astype(f32) + total[s, :].astype(bf16).astype(f32)).astype(bf16)
        H[s, :] = h
        A[s, :] = normed(h.astype(f32))
        total[s, :] = jnp.zeros((rb, D), f32)
        return 0

    with jax.named_scope('between'):
        lax.fori_loop(0, T // rb, between, 0)
    with jax.named_scope('p_one'):
        phase(CHUNKS, True, True)
    load_a = pltpu.make_async_copy(a0_hbm, A, in_sem.at[0])
    load_a.start()

    def back(t, _):
        s = tile(t, rb)
        wide = H[s, :].astype(f32)
        da = total[s, :].astype(bf16).astype(f32)
        scale = lax.rsqrt(jnp.mean(wide * wide, -1, keepdims=True) + 1e-6)
        along = jnp.sum(da * wide, -1, keepdims=True) * (scale * scale * scale * (1.0 / D))
        dn = (da * scale - wide * along).astype(bf16).astype(f32)
        DH[s, :] = (DH[s, :].astype(f32) + dn).astype(bf16)
        return 0

    with jax.named_scope('back'):
        lax.fori_loop(0, T // rb, back, 0)
        load_a.wait()
    block = T // (4 * CHUNKS)
    fetch = list(zip(early, early_out))
    for i, w in enumerate((wg_hbm, wu_hbm)):
        for l in range(2):
            for k in range(CHUNKS):
                there = H.at[pl.ds(((2 * i + l) * CHUNKS + k) * block, block), :]
                fetch.append((w.at[l, :, pl.ds(k * F, F)], there))
    fetch = [pltpu.make_async_copy(src, dst, early_sem.at[i]) for i, (src, dst) in enumerate(fetch)]
    for copy in fetch:
        copy.start()
    with jax.named_scope('p_zero'):
        phase(2 * CHUNKS, True, False)

    with jax.named_scope("drain"):
        drain()
    with jax.named_scope("norm"):
        mean = jnp.sum(over_s[...]) * (1.0 / COUNT)
        factor[...] = jnp.minimum(1.0, 0.5 * lax.rsqrt(jnp.full(factor.shape, mean + 1e-30, f32)))

    def finish(q, _):
        l, j = q // CHUNKS, lax.rem(q, CHUNKS)
        one = wbuf.at[l, j, :, :R, :]
        remote(one, one, ws_send.at[1, q], w_recv.at[1, q + 2], to_partner).wait_send()
        one = wbuf.at[l, j, :, :HALF, :]
        remote(one, one, ws_send.at[0, q], w_recv.at[0, q + 2], to_across).wait_send()

        @pl.when(q > 0)
        def _():
            for kind in (2, 3, 4):
                pass_on(kind, q, across, my, to_partner).wait_send()

        return 0

    for copy in fetch:
        copy.wait()
    with jax.named_scope('finish'):
        lax.fori_loop(0, last, finish, 0)


def gradients_of(x, dy, w_gate, w_up, w_down, early, tiles=(512, 256, 256), vmem=39 * 2**20):
    T, D = x.shape
    F = w_gate.shape[2] // CHUNKS
    Tt, rb, cb = tiles
    R = D // OWNERS
    H, Q = R // YS, R // (YS * ZS)
    n = 2 * CHUNKS
    lanes = min(F, 128)
    vm = pltpu.VMEM
    dma, hbm = pltpu.SemaphoreType.DMA, pl.BlockSpec(memory_space=pltpu.HBM)
    outs = pl.pallas_call(
        functools.partial(kernel, (T, D, F, Tt, rb, cb, lanes)),
        in_specs=[hbm] * (5 + len(early)),
        out_specs=[hbm, pl.BlockSpec(memory_space=pltpu.VMEM), hbm, hbm] + [pl.BlockSpec(memory_space=pltpu.VMEM)] * 6,
        out_shape=[
            pltpu.HBM((n, 3, R, F), bf16), pltpu.VMEM((8, 128), f32),
            pltpu.HBM((2, CHUNKS, 3, D, F), bf16), pltpu.HBM((T, D), bf16),
            *(pltpu.VMEM(a.shape, a.dtype) for a in early), pltpu.VMEM((T, D), bf16),
        ],
        scratch_shapes=[
            vm((T, D), bf16), vm((T, D), bf16), vm((T, D), f32),
            vm((2, 3, D, F), bf16), vm((2, Tt, F), bf16), vm((2, Tt, F), bf16), vm((2, Tt, F), bf16), vm((3, D, F), f32),
            vm((3, XS, R, F), bf16), vm((2, 3, XS, R, F), bf16), vm((3, XS, R, F), f32),
            vm((3, R, F), bf16), vm((2, 3, R, F), bf16), vm((3, R, F), f32),
            vm((3, H, F), bf16), vm((2, 3, H, F), bf16), vm((3, H, F), f32),
            vm((3, ZS - 1, Q, F), bf16), vm((2, 3, ZS - 1, Q, F), bf16), vm((3, Q, F), f32),
            vm((n, 3, Q, F), bf16), vm((Q, lanes), f32), vm((YS * ZS, Q, lanes), f32), vm((OWNERS, Q, lanes), f32),
            dma((2,)), dma((5 + 4 * CHUNKS,)), dma((2,)), dma, dma((2, 3)),
            dma((2, n)), dma((3, n + 2)), dma((5, n + 2)),
            dma((3,)), dma((2, 3)), dma((3,)), dma((2, 3)), dma((3,)), dma((2, 3)), dma((3, ZS - 1)), dma((2, 3, ZS - 1)), dma((2, 3)), dma((2, 3)), dma((2, 3)), dma((2, 3)),
            dma((YS * ZS - 1,)), dma((YS * ZS - 1,)), dma((OWNERS - 1,)), dma((OWNERS - 1,)),
        ],
        compiler_params=pltpu.CompilerParams(collective_id=0, has_side_effects=True, vmem_limit_bytes=vmem),
    )(*(pltpu.with_memory_space_constraint(a, pltpu.HBM) for a in (x, dy, w_gate, w_up, w_down, *early)))
    return outs[0], outs[1], outs[4:]


def update(factor, ga, gb, gc, m_gate, m_up, m_down, v_gate, v_up, H, w_down, v_down, *outs):
    l, o = pl.program_id(0), pl.program_id(1)
    scale = factor[0:1, 0:1]
    for i, g in enumerate((ga, gb, gc)):
        _, parts, _, R, wide = g.shape
        for j in range(parts):
            if i < 2:
                near = (slice(None), slice(j * wide, (j + 1) * wide))
                far = (l, slice(None), pl.ds(pl.multiple_of((o * parts + j) * wide, wide), wide))
                m, v = (m_gate, m_up)[i][far], (v_gate, v_up)[i][far]
                row = ((2 * i + l) * CHUNKS + 2 * o + j // OWNERS) * R
                w = H[pl.ds(pl.multiple_of(row, R), R), (j % OWNERS) * wide : (j % OWNERS + 1) * wide]
            else:
                near = (slice(j * R, (j + 1) * R), slice(None))
                row = (o * parts + j) * R
                w = w_down[0, *near]
                m = m_down[l, pl.ds(pl.multiple_of(row, R), R), :]
                v = v_down[0, *near]
            gradient = g[0, j, 0].astype(f32) * scale
            w = w.astype(f32)
            m = 0.9 * m + 0.1 * gradient
            v = 0.95 * v + 0.05 * gradient * gradient
            outs[i][0, *near] = (w - 0.02 * (m * lax.rsqrt(v + 1e-8) + 0.1 * w)).astype(bf16)
            outs[3 + i][0, *near] = m
            outs[6 + i][0, *near] = v


def updated(g, factor, early, late, like):
    _, _, _, R, F = g.shape
    wide = F // OWNERS
    at = pl.BlockSpec
    native = [at((1, R, CHUNKS * wide), lambda l, o: (l, 0, o))] * 2 + [at((1, CHUNKS * R // OWNERS, F), lambda l, o: (l, o, 0))]
    mine = [at((1, CHUNKS, 1, R, wide), lambda l, o, k=k: (1 - l, 0, k, 0, o)) for k in range(2)]
    mine.append(at((1, CHUNKS // OWNERS, 1, R, F), lambda l, o: (1 - l, o, 2, 0, 0)))
    g = pltpu.with_memory_space_constraint(g, pltpu.HBM)
    early = [pltpu.with_memory_space_constraint(a, pltpu.VMEM) for a in early]
    return pl.pallas_call(
        update,
        grid=(2, OWNERS),
        in_specs=[at((8, 128), lambda l, o: (0, 0)), *mine, *[at(memory_space=pltpu.VMEM)] * len(early), native[2], native[2]],
        out_specs=native * 3,
        out_shape=[jax.ShapeDtypeStruct(a.shape, a.dtype) for a in like],
        compiler_params=pltpu.CompilerParams(vmem_limit_bytes=14 * 2**20),
    )(factor, g, g, g, *early, *(pltpu.with_memory_space_constraint(a, pltpu.HBM) for a in late))


def solution(mesh, **options):
    def step(x, dy, *arrays):
        weights, m, v = (arrays[i : i + 3] for i in (0, 3, 6))
        g, factor, early = gradients_of(x[0], dy[0], *weights, [*m, *v[:2]], **options)
        return tuple(updated(g.reshape(2, CHUNKS, *g.shape[1:]), factor, early, (weights[2], v[2]), arrays))

    states, cut = P(("rep", "r", "s"), None, None), P(None, "s", None)
    return jax.shard_map(
        step,
        mesh=mesh,
        in_specs=(states, states) + (cut,) * 9,
        out_specs=(P("rep", "s", None),) * 9,
        check_vma=False,
    )
```

```python
import functools

import jax
import jax.numpy as jnp
from jax import lax
from jax.experimental import pallas as pl
from jax.experimental.pallas import tpu as pltpu
from jax.sharding import PartitionSpec as P

MESH = pl.DeviceIdType.MESH
CHUNKS, CORES, XS, YS, ZS, OWNERS = 8, 2, 2, 2, 4, 4
FIRST = 0
f32, bf16 = jnp.float32, jnp.bfloat16

def dotn(a, b):
    return jnp.dot(a, b, preferred_element_type=f32)


def dott(a, b):
    return lax.dot_general(a, b, (((1,), (1,)), ((), ())), preferred_element_type=f32)


def dot0(a, b):
    return lax.dot_general(a, b, (((0,), (0,)), ((), ())), preferred_element_type=f32)


def kernel(
    sizes,
    x_hbm, dy_hbm, wg_hbm, wu_hbm, wd_hbm, *refs,
):
    early, refs = refs[:5], refs[5:]
    kernel_(sizes, x_hbm, dy_hbm, wg_hbm, wu_hbm, wd_hbm, early, refs[4:9], *refs[:4], *refs[9:])


def kernel_(
    sizes,
    x_hbm, dy_hbm, wg_hbm, wu_hbm, wd_hbm, early, early_out, gfin, factor, wbuf, a0_hbm,
    H, A, DH, total, W, act_s, du_s, dg_s, accs,
    sb0, rb0, own0, sb1, rb1, own1, sb2, rb2, own2, sb3, rb3, own3, piece, squares, over_r, over_s,
    in_sem, early_sem, w_sem, keep_sem, out_sem,
    ws_send, wf_send, w_recv,
    s0, r0, s1, r1, s2, r2, s3, r3, s4, r4, s5, r5, sn, rn, sm, rm,
):
    T, D, F, Tt, rb, cb, LANES = sizes
    COUNT = 2 * CHUNKS * 3 * D * F
    R = D // OWNERS
    HALF, QUARTER = R // YS, R // (YS * ZS)
    nt = T // Tt
    per = nt // 2
    me_r, me_s = lax.axis_index("r"), lax.axis_index("s")
    core, mx = lax.rem(me_s, CORES), me_s // CORES
    my, mz = me_r // ZS, lax.rem(me_r, ZS)
    partner = mx * CORES + 1 - core
    across = (1 - mx) * CORES + core
    to_partner = {"r": me_r, "s": partner}
    to_across = {"r": me_r, "s": across}
    to_y = {"r": (1 - my) * ZS + mz, "s": me_s}

    def remote(src, dst, send, recv, where):
        return pltpu.make_async_remote_copy(src, dst, send, recv, device_id=where, device_id_type=MESH)

    def rows(owner):
        return pl.ds(pl.multiple_of(owner * R, R), R)

    def half(h):
        return pl.ds(pl.multiple_of(h * HALF, HALF), HALF)

    def part_of(owner, h):
        return pl.ds(pl.multiple_of(owner * R + h * HALF, HALF), HALF)

    def own_pieces(l, j, into, h=None):
        wide = F // OWNERS
        there = rows(me_s) if h is None else part_of(me_s, h)
        for m, w in ((0, wg_hbm), (1, wu_hbm)):
            for o in range(OWNERS):
                cols = pl.ds(pl.multiple_of(o * wide * CHUNKS + j * wide, wide), wide)
                src = w.at[l, :, cols] if h is None else w.at[l, half(h), cols]
                yield m, src, into.at[m, there, o * wide : (o + 1) * wide]
        here = rows(j) if h is None else part_of(j, h)
        yield 2, wd_hbm.at[l, here, :], into.at[2, there, :]

    def chunk_of(c):
        return c // CHUNKS, lax.rem(c, CHUNKS)

    def send_own(c):
        l, j = chunk_of(c)
        into = W.at[0] if c is FIRST else wbuf.at[l, j]
        for m, src, dst in own_pieces(l, j, into, my):
            at = m if c is FIRST else c + 2
            remote(src, dst, ws_send.at[0, c], w_recv.at[0, at], to_across).start()
        for m, src, dst in own_pieces(l, j, into):
            remote(src, dst, ws_send.at[1, c], w_recv.at[1, c + 2], to_partner).start()

    def pass_on(kind, c, owner, h, where, m=None):
        l, j = chunk_of(c)
        part = wbuf.at[l, j, :, part_of(owner, h), :] if m is None else W.at[0, m, part_of(owner, h), :]
        at = c + 2 if m is None else m
        return remote(part, part, wf_send.at[max(kind - 2, 0), at], w_recv.at[kind, at], where)

    def forward(c, m=None):
        pass_on(0, c, across, my, to_across, m).wait_recv()
        pass_on(3, c, across, my, to_y, m).start()
        pass_on(2, c, across, my, to_partner, m).start()

    def forward2(c, m=None):
        pass_on(3, c, across, 1 - my, to_y, m).wait_recv()
        pass_on(4, c, across, 1 - my, to_partner, m).start()

    def load(n):
        slot = lax.rem(n, 2)
        l, j = lax.rem(n // CHUNKS, 2), lax.rem(n, CHUNKS)

        @pl.when(n < 2 * CHUNKS)
        def _():
            whole = wbuf.at[l, j, :, rows(partner), :]
            remote(whole, whole, ws_send.at[1, n], w_recv.at[1, n + 2], to_partner).wait_recv()
            pass_on(2, n, partner, my, to_partner).wait_recv()
            pass_on(4, n, partner, 1 - my, to_partner).wait_recv()

        for _, src, dst in own_pieces(l, j, W.at[slot]):
            pltpu.make_async_copy(src, dst, w_sem.at[slot]).start()
        for k in range(1, OWNERS):
            o = lax.rem(me_s + k, OWNERS)
            pltpu.make_async_copy(wbuf.at[l, j, :, rows(o), :], W.at[slot, :, rows(o), :], w_sem.at[slot]).start()

    def load_first():
        for _, src, dst in own_pieces(0, 0, W.at[0]):
            pltpu.make_async_copy(src, dst, w_sem.at[0]).start()

    def wait_first():
        mine = W.at[0, :, rows(me_s), :]
        pltpu.make_async_copy(mine, mine, w_sem.at[0]).wait()
        whole = W.at[0, :, rows(partner), :]
        remote(whole, whole, ws_send.at[1, 0], w_recv.at[1, 2], to_partner).wait_recv()
        for m in range(3):
            pass_on(2, FIRST, partner, my, to_partner, m).wait_recv()
            pass_on(4, FIRST, partner, 1 - my, to_partner, m).wait_recv()

    def keep_first():
        return pltpu.make_async_copy(W.at[0], wbuf.at[0, 0], keep_sem)

    def free_first(_):
        keep_first().wait()
        for m in range(3):
            for kind in (2, 3, 4):
                pass_on(kind, FIRST, across, my, to_partner, m).wait_send()

    def wait_load(n):
        slot = lax.rem(n, 2)
        pltpu.make_async_copy(wbuf.at[0, 0], W.at[slot], w_sem.at[slot]).wait()

    def c0(q, m):
        slot = lax.rem(q, 2)
        return remote(sb0.at[m], rb0.at[slot, m], s0.at[m], r0.at[slot, m], to_partner)

    def g0(q, m):
        for xx in range(XS):
            sb0[m, xx] = accs[m, rows(xx * CORES + 1 - core), :].astype(bf16)
        for xx in range(XS):
            own0[m, xx] = accs[m, rows(xx * CORES + core), :]
        c0(q, m).start()

    def c1(q, m):
        slot = lax.rem(q, 2)
        return remote(sb1.at[m], rb1.at[slot, m], s1.at[m], r1.at[slot, m], to_across)

    def g1(q, m):
        c0(q, m).wait()
        slot = lax.rem(q, 2)
        sb1[m] = (own0[m, 1 - mx] + rb0[slot, m, 1 - mx].astype(f32)).astype(bf16)
        own1[m] = own0[m, mx] + rb0[slot, m, mx].astype(f32)
        c1(q, m).start()

    def c2(q, m):
        slot = lax.rem(q, 2)
        return remote(sb2.at[m], rb2.at[slot, m], s2.at[m], r2.at[slot, m], to_y)

    def g2(q, m):
        c1(q, m).wait()
        slot = lax.rem(q, 2)
        sb2[m] = (own1[m, half(1 - my), :] + rb1[slot, m, half(1 - my), :].astype(f32)).astype(bf16)
        own2[m] = own1[m, half(my), :] + rb1[slot, m, half(my), :].astype(f32)
        c2(q, m).start()

    def quarter(z):
        return pl.ds(pl.multiple_of(z * QUARTER, QUARTER), QUARTER)

    def c3(q, m, k):
        where = {"r": my * ZS + lax.rem(mz + 1 + k, ZS), "s": me_s}
        slot = lax.rem(q, 2)
        return remote(sb3.at[m, k], rb3.at[slot, m, k], s3.at[m, k], r3.at[slot, m, k], where)

    def g3(q, m):
        c2(q, m).wait()
        slot = lax.rem(q, 2)
        for k in range(ZS - 1):
            z = lax.rem(mz + 1 + k, ZS)
            sb3[m, k] = (own2[m, quarter(z), :] + rb2[slot, m, quarter(z), :].astype(f32)).astype(bf16)
        own3[m] = own2[m, quarter(mz), :] + rb2[slot, m, quarter(mz), :].astype(f32)
        for k in range(ZS - 1):
            c3(q, m, k).start()

    mine = pl.ds(pl.multiple_of(my * HALF + mz * QUARTER, QUARTER), QUARTER)

    def to_peer(k):
        return {"r": lax.rem(me_r + 1 + k, YS * ZS), "s": me_s}

    def c4(q, m, k):
        where = {"r": my * ZS + lax.rem(mz + 1 + k, ZS), "s": me_s}
        return remote(piece.at[q, m], gfin.at[q, m, mine, :], s4.at[lax.rem(q, 2), m], r4.at[lax.rem(q, 2), m], where)

    def c4_here(q, m):
        return pltpu.make_async_copy(piece.at[q, m], gfin.at[q, m, mine, :], out_sem.at[lax.rem(q, 2), m])

    def g4(q, m, then=None):
        slot = lax.rem(q, 2)
        for k in range(ZS - 1):
            c3(q, m, k).wait()
        v = own3[m]
        for k in range(ZS - 1):
            v += rb3[slot, m, k].astype(f32)
        v = v.astype(bf16)
        piece[q, m] = v
        v = v.astype(f32)
        squares[...] += sum(v[:, i : i + LANES] * v[:, i : i + LANES] for i in range(0, F, LANES))
        if then is not None:
            then()
        for k in range(ZS - 1):
            c4(q, m, k).start()
        c4_here(q, m).start()

    def c5(q, m):
        part = gfin.at[q, m, half(my), :]
        return remote(part, part, s5.at[lax.rem(q, 2), m], r5.at[lax.rem(q, 2), m], to_y)

    def g5(q, m):
        others = gfin.at[q, m, : HALF - QUARTER, :]
        remote(others, others, s4.at[lax.rem(q, 2), m], r4.at[lax.rem(q, 2), m], to_y).wait()
        c4_here(q, m).wait()
        c5(q, m).start()

    def g6(q, m):
        c5(q, m).wait()

    def each(stage, which=(0, 1, 2)):
        def run(q):
            for m in which:
                stage(q, m)

        run.__name__ = stage.__name__
        return run

    def when(test, what, q):
        def run():
            with jax.named_scope(what.__name__):
                what(q)
        pl.when(test)(run)

    last = 2 * CHUNKS

    def exchange(q, b):
        def at(stage, *parts):
            @pl.when(b == stage)
            def _():
                for back, what, which in parts:
                    when(q >= back, each(what, which), q - back)

        every = (0, 1, 2)
        at(0, (2, g2, (2,)), (1, g0, every), (3, g4, (2,)), (4, g6, every))
        at(1, (1, g1, every), (2, g3, (0, 1)), (3, g5, (0, 1)))
        at(2, (2, g3, (2,)), (3, g5, (2,)))
        at(3, (1, g2, (0, 1)), (2, g4, (0, 1)))

    def drain():
        a, b, c = last - 3, last - 2, last - 1
        each(g0)(c)
        g2(b, 2)
        each(g6)(a - 1)
        g4(a, 2)
        each(g3, (0, 1))(b)
        each(g1)(c)
        each(g5, (0, 1))(a)
        g3(b, 2)
        each(g4, (0, 1))(b)
        g5(a, 2)
        g2(c, 0)
        g4(b, 2)
        each(g6)(a)
        g2(c, 1)
        g3(c, 0)
        each(g5, (0, 1))(b)
        g2(c, 2)
        g3(c, 1)
        g5(b, 2)
        g4(c, 0)
        g3(c, 2)
        g4(c, 1)
        each(g6)(b)
        g5(c, 0)
        peers_r = [to_peer(k) for k in range(YS * ZS - 1)]
        from_r = [lax.rem(me_r + YS * ZS - 1 - k, YS * ZS) for k in range(YS * ZS - 1)]
        peers_s = [{"r": me_r, "s": lax.rem(me_s + 1 + k, OWNERS)} for k in range(OWNERS - 1)]
        from_s = [lax.rem(me_s + OWNERS - 1 - k, OWNERS) for k in range(OWNERS - 1)]

        def tell_squares():
            over_r[me_r] = squares[...]
            tell(me_r, over_r, sn, rn, peers_r)

        g4(c, 2, tell_squares)
        g5(c, 1)
        hear(me_r, over_r, sn, rn, peers_r, from_r)
        over_s[me_s] = jnp.sum(over_r[...], 0)
        tell(me_s, over_s, sm, rm, peers_s)
        g5(c, 2)
        hear(me_s, over_s, sm, rm, peers_s, from_s)
        each(g6)(c)

    def tell(me, scratch, send, recv, others):
        for k, where in enumerate(others):
            remote(scratch.at[me], scratch.at[me], send.at[k], recv.at[k], where).start()

    def hear(me, scratch, send, recv, others, places):
        for k, (where, place) in enumerate(zip(others, places)):
            remote(scratch.at[me], scratch.at[place], send.at[k], recv.at[k], where).wait()

    def normed(wide):
        scale = lax.rsqrt(jnp.mean(wide * wide, -1, keepdims=True) + 1e-6)
        return (wide * scale).astype(bf16)

    def tile(t, n=Tt):
        return pl.ds(pl.multiple_of(t * n, n), n)

    def first(wslot, t, slot, backward, r, c):
        s = pl.ds(pl.multiple_of(t * Tt + r * rb, rb), rb)
        rs, cs = slice(r * rb, (r + 1) * rb), slice(c * cb, (c + 1) * cb)
        a = A[s, :]
        g = dotn(a, W[wslot, 0, :, cs])
        u = dotn(a, W[wslot, 1, :, cs])
        h = 0.5 * g
        th = jnp.tanh(h)
        silu = h * th + h
        if not backward:
            act_s[slot, rs, cs] = (silu * u).astype(bf16)
            return
        d = dott(DH[s, :], W[wslot, 2, cs, :]).astype(bf16).astype(f32)
        sig = 0.5 * th + 0.5
        act_s[slot, rs, cs] = (silu * u).astype(bf16)
        du_s[slot, rs, cs] = (d * silu).astype(bf16)
        dg_s[slot, rs, cs] = (d * u * (sig * (1.0 + g - silu))).astype(bf16)

    def second(wslot, t, slot, backward, input_too, begin, which):
        s = tile(t)
        if not backward:
            total[s, :] += dotn(act_s[slot], W[wslot, 2])
            return
        if which == 3:
            total[s, :] += dott(dg_s[slot], W[wslot, 0]) + dott(du_s[slot], W[wslot, 1])
            return
        if which == 2:
            new = dot0(act_s[slot], DH[s, :])
        else:
            new = dot0(A[s, :], (dg_s, du_s)[which][slot])
        if begin:
            accs[which] = jnp.where(t == 0, 0.0, accs[which]) + new
        else:
            accs[which] += new

    blocks = [(r, c) for r in range(Tt // rb) for c in range(F // cb)]

    def together(w1, t1, slot1, w2, t2, slot2, backward, input_too, begin, ahead=True):
        for which in range(4 if input_too else 3) if backward else [0]:
            second(w2, t2, slot2, backward, input_too, begin, which)
        for block in blocks if ahead else ():
            first(w1, t1, slot1, backward, *block)

    def phase(base, backward, input_too):
        for block in blocks:
            first(lax.rem(base, 2), 0, 0, backward, *block)

        def step(final, i, _):
            n, b = base + i // per, lax.rem(i, per)
            if backward:
                exchange(n - CHUNKS, b)
            if base < 2 * CHUNKS:

                @pl.when(b == 0)
                def _():
                    when(n + 4 < 2 * CHUNKS, send_own, n + 4)

                @pl.when(b == 1)
                def _():
                    when(n + 1 < 2 * CHUNKS, forward2, n + 1)
                    when(n + 2 < 2 * CHUNKS, forward, n + 2)
                    when(n == 1, free_first, n)

            when((b == 2) & (n + 1 < 3 * CHUNKS), load, n + 1)
            when((b == per - 1) & (n + 1 < 3 * CHUNKS), wait_load, n + 1)
            w = lax.rem(n, 2)
            t = 2 * b
            together(w, t + 1, 1, w, t, 0, backward, input_too, True)
            over = b == per - 1
            together(jnp.where(over, 1 - w, w), jnp.where(over, 0, t + 2), 0, w, t + 1, 1, backward, input_too, False, not final)
            return 0

        lax.fori_loop(0, per * CHUNKS - 1, functools.partial(step, False), 0)
        lax.fori_loop(per * CHUNKS - 1, per * CHUNKS, functools.partial(step, True), 0)

    barrier = pltpu.get_barrier_semaphore()
    peers = [to_partner, to_across] + [{"r": lax.rem(me_r + k, YS * ZS), "s": me_s} for k in range(1, YS * ZS)]
    for peer in peers:
        pl.semaphore_signal(barrier, inc=1, device_id=peer, device_id_type=MESH)
    load_x = pltpu.make_async_copy(x_hbm, H, in_sem.at[0])
    load_dy = pltpu.make_async_copy(dy_hbm, DH, in_sem.at[1])
    load_x.start()
    load_dy.start()
    with jax.named_scope('barrier'):
        pl.semaphore_wait(barrier, len(peers))
    send_own(FIRST)
    load_first()
    lax.fori_loop(1, 4, lambda c, _: (send_own(c), 0)[1], 0)
    load_x.wait()

    def begin(t, _):
        s = tile(t, rb)
        A[s, :] = normed(H[s, :].astype(f32))
        total[s, :] = jnp.zeros((rb, D), f32)
        return 0

    squares[...] = jnp.zeros(squares.shape, f32)
    with jax.named_scope('begin'):
        lax.fori_loop(0, T // rb, begin, 0)
    save_a = pltpu.make_async_copy(A, a0_hbm, in_sem.at[0])
    save_a.start()
    with jax.named_scope('first_load'):
        for m in range(3):
            forward(FIRST, m)
        for m in range(3):
            forward2(FIRST, m)
        forward(1)
        wait_first()
        keep_first().start()
    with jax.named_scope('p_fwd'):
        phase(0, False, False)
    save_a.wait()
    load_dy.wait()

    def between(t, _):
        s = tile(t, rb)
        h = (H[s, :].astype(f32) + total[s, :].astype(bf16).astype(f32)).astype(bf16)
        H[s, :] = h
        A[s, :] = normed(h.astype(f32))
        total[s, :] = jnp.zeros((rb, D), f32)
        return 0

    with jax.named_scope('between'):
        lax.fori_loop(0, T // rb, between, 0)
    with jax.named_scope('p_one'):
        phase(CHUNKS, True, True)
    load_a = pltpu.make_async_copy(a0_hbm, A, in_sem.at[0])
    load_a.start()

    def back(t, _):
        s = tile(t, rb)
        wide = H[s, :].astype(f32)
        da = total[s, :].astype(bf16).astype(f32)
        scale = lax.rsqrt(jnp.mean(wide * wide, -1, keepdims=True) + 1e-6)
        along = jnp.sum(da * wide, -1, keepdims=True) * (scale * scale * scale * (1.0 / D))
        dn = (da * scale - wide * along).astype(bf16).astype(f32)
        DH[s, :] = (DH[s, :].astype(f32) + dn).astype(bf16)
        return 0

    with jax.named_scope('back'):
        lax.fori_loop(0, T // rb, back, 0)
        load_a.wait()
    block = T // (4 * CHUNKS)
    fetch = list(zip(early, early_out))
    for i, w in enumerate((wg_hbm, wu_hbm)):
        for l in range(2):
            for k in range(CHUNKS):
                there = H.at[pl.ds(((2 * i + l) * CHUNKS + k) * block, block), :]
                fetch.append((w.at[l, :, pl.ds(k * F, F)], there))
    fetch = [pltpu.make_async_copy(src, dst, early_sem.at[i]) for i, (src, dst) in enumerate(fetch)]
    for copy in fetch:
        copy.start()
    with jax.named_scope('p_zero'):
        phase(2 * CHUNKS, True, False)

    with jax.named_scope("drain"):
        drain()
    with jax.named_scope("norm"):
        mean = jnp.sum(over_s[...]) * (1.0 / COUNT)
        factor[...] = jnp.minimum(1.0, 0.5 * lax.rsqrt(jnp.full(factor.shape, mean + 1e-30, f32)))

    def finish(q, _):
        l, j = q // CHUNKS, lax.rem(q, CHUNKS)
        one = wbuf.at[l, j, :, :R, :]
        remote(one, one, ws_send.at[1, q], w_recv.at[1, q + 2], to_partner).wait_send()
        one = wbuf.at[l, j, :, :HALF, :]
        remote(one, one, ws_send.at[0, q], w_recv.at[0, q + 2], to_across).wait_send()

        @pl.when(q > 0)
        def _():
            for kind in (2, 3, 4):
                pass_on(kind, q, across, my, to_partner).wait_send()

        return 0

    for copy in fetch:
        copy.wait()
    with jax.named_scope('finish'):
        lax.fori_loop(0, last, finish, 0)


def gradients_of(x, dy, w_gate, w_up, w_down, early, tiles=(512, 256, 256), vmem=39 * 2**20):
    T, D = x.shape
    F = w_gate.shape[2] // CHUNKS
    Tt, rb, cb = tiles
    R = D // OWNERS
    H, Q = R // YS, R // (YS * ZS)
    n = 2 * CHUNKS
    lanes = min(F, 128)
    vm = pltpu.VMEM
    dma, hbm = pltpu.SemaphoreType.DMA, pl.BlockSpec(memory_space=pltpu.HBM)
    outs = pl.pallas_call(
        functools.partial(kernel, (T, D, F, Tt, rb, cb, lanes)),
        in_specs=[hbm] * (5 + len(early)),
        out_specs=[hbm, pl.BlockSpec(memory_space=pltpu.VMEM), hbm, hbm] + [pl.BlockSpec(memory_space=pltpu.VMEM)] * 6,
        out_shape=[
            pltpu.HBM((n, 3, R, F), bf16), pltpu.VMEM((8, 128), f32),
            pltpu.HBM((2, CHUNKS, 3, D, F), bf16), pltpu.HBM((T, D), bf16),
            *(pltpu.VMEM(a.shape, a.dtype) for a in early), pltpu.VMEM((T, D), bf16),
        ],
        scratch_shapes=[
            vm((T, D), bf16), vm((T, D), bf16), vm((T, D), f32),
            vm((2, 3, D, F), bf16), vm((2, Tt, F), bf16), vm((2, Tt, F), bf16), vm((2, Tt, F), bf16), vm((3, D, F), f32),
            vm((3, XS, R, F), bf16), vm((2, 3, XS, R, F), bf16), vm((3, XS, R, F), f32),
            vm((3, R, F), bf16), vm((2, 3, R, F), bf16), vm((3, R, F), f32),
            vm((3, H, F), bf16), vm((2, 3, H, F), bf16), vm((3, H, F), f32),
            vm((3, ZS - 1, Q, F), bf16), vm((2, 3, ZS - 1, Q, F), bf16), vm((3, Q, F), f32),
            vm((n, 3, Q, F), bf16), vm((Q, lanes), f32), vm((YS * ZS, Q, lanes), f32), vm((OWNERS, Q, lanes), f32),
            dma((2,)), dma((5 + 4 * CHUNKS,)), dma((2,)), dma, dma((2, 3)),
            dma((2, n)), dma((3, n + 2)), dma((5, n + 2)),
            dma((3,)), dma((2, 3)), dma((3,)), dma((2, 3)), dma((3,)), dma((2, 3)), dma((3, ZS - 1)), dma((2, 3, ZS - 1)), dma((2, 3)), dma((2, 3)), dma((2, 3)), dma((2, 3)),
            dma((YS * ZS - 1,)), dma((YS * ZS - 1,)), dma((OWNERS - 1,)), dma((OWNERS - 1,)),
        ],
        compiler_params=pltpu.CompilerParams(collective_id=0, has_side_effects=True, vmem_limit_bytes=vmem),
    )(*(pltpu.with_memory_space_constraint(a, pltpu.HBM) for a in (x, dy, w_gate, w_up, w_down, *early)))
    return outs[0], outs[1], outs[4:]


def update(factor, ga, gb, gc, m_gate, m_up, m_down, v_gate, v_up, H, w_down, v_down, *outs):
    l, o = pl.program_id(0), pl.program_id(1)
    scale = factor[0:1, 0:1]
    for i, g in enumerate((ga, gb, gc)):
        _, parts, _, R, wide = g.shape
        for j in range(parts):
            if i < 2:
                near = (slice(None), slice(j * wide, (j + 1) * wide))
                far = (l, slice(None), pl.ds(pl.multiple_of((o * parts + j) * wide, wide), wide))
                m, v = (m_gate, m_up)[i][far], (v_gate, v_up)[i][far]
                row = ((2 * i + l) * CHUNKS + 2 * o + j // OWNERS) * R
                w = H[pl.ds(pl.multiple_of(row, R), R), (j % OWNERS) * wide : (j % OWNERS + 1) * wide]
            else:
                near = (slice(j * R, (j + 1) * R), slice(None))
                row = (o * parts + j) * R
                w = w_down[0, *near]
                m = m_down[l, pl.ds(pl.multiple_of(row, R), R), :]
                v = v_down[0, *near]
            gradient = g[0, j, 0].astype(f32) * scale
            w = w.astype(f32)
            m = 0.9 * m + 0.1 * gradient
            v = 0.95 * v + 0.05 * gradient * gradient
            outs[i][0, *near] = (w - 0.02 * (m * lax.rsqrt(v + 1e-8) + 0.1 * w)).astype(bf16)
            outs[3 + i][0, *near] = m
            outs[6 + i][0, *near] = v


def updated(g, factor, early, late, like):
    _, _, _, R, F = g.shape
    wide = F // OWNERS
    at = pl.BlockSpec
    native = [at((1, R, CHUNKS * wide), lambda l, o: (l, 0, o))] * 2 + [at((1, CHUNKS * R // OWNERS, F), lambda l, o: (l, o, 0))]
    mine = [at((1, CHUNKS, 1, R, wide), lambda l, o, k=k: (1 - l, 0, k, 0, o)) for k in range(2)]
    mine.append(at((1, CHUNKS // OWNERS, 1, R, F), lambda l, o: (1 - l, o, 2, 0, 0)))
    g = pltpu.with_memory_space_constraint(g, pltpu.HBM)
    early = [pltpu.with_memory_space_constraint(a, pltpu.VMEM) for a in early]
    return pl.pallas_call(
        update,
        grid=(2, OWNERS),
        in_specs=[at((8, 128), lambda l, o: (0, 0)), *mine, *[at(memory_space=pltpu.VMEM)] * len(early), native[2], native[2]],
        out_specs=native * 3,
        out_shape=[jax.ShapeDtypeStruct(a.shape, a.dtype) for a in like],
        compiler_params=pltpu.CompilerParams(vmem_limit_bytes=14 * 2**20),
    )(factor, g, g, g, *early, *(pltpu.with_memory_space_constraint(a, pltpu.HBM) for a in late))


def solution(mesh, **options):
    def step(x, dy, *arrays):
        weights, m, v = (arrays[i : i + 3] for i in (0, 3, 6))
        g, factor, early = gradients_of(x[0], dy[0], *weights, [*m, *v[:2]], **options)
        return tuple(updated(g.reshape(2, CHUNKS, *g.shape[1:]), factor, early, (weights[2], v[2]), arrays))

    states, cut = P(("rep", "r", "s"), None, None), P(None, "s", None)
    return jax.shard_map(
        step,
        mesh=mesh,
        in_specs=(states, states) + (cut,) * 9,
        out_specs=(P("rep", "s", None),) * 9,
        check_vma=False,
    )
```
